256 devices in a mesh: grp: 4 (over x), gx: 16 (over z, core), gy: 4 (over y).
Axes of the slice: x: 4, y: 4, z: 8, core: 2. Of those that a mesh axis runs over, the one named last changes fastest.
Arguments:
- conserved: float32 [8, 4, 128, 64, 128], P(None, 'grp', 'gx', 'gy'), may hold values from -6 to 6
- velocity: float32 [3, 4, 128, 64, 128], P(None, 'grp', 'gx', 'gy'), may hold values from -0.45 to 0.45
- donor_corner: int32 [4, 16, 4, 4, 64, 32], P('grp', 'gx', 'gy'), may hold values from 0 to 14206, as said below
- donor_fraction: float32 [3, 4, 16, 4, 4, 64, 32], P(None, 'grp', 'gx', 'gy'), may hold values from 0 to 1
- target_cell: int32 [4, 16, 4, 4, 64, 32], P('grp', 'gx', 'gy'), may hold values from 0 to 16384, as said below
Outputs:
- advanced: float32 [8, 4, 128, 64, 128], P(None, 'grp', 'gx', 'gy')
The draws below stay inside these ranges and needn't reach their ends.
Inputs may be any that keep to these rules, and one draw needn't show every extreme that they name: `donor_corner`: each used slot's stencil lies inside the donor device's block (x < 7, y < 15, z < 127); entries of empty slots are 0. Slot s of a pair is used exactly when s is below that pair's count, the same count as in target_cell; a pair's count is at most 32; every device fills 32 slots on the device of the same index in the grid two further on (grid indices modulo 4); devices of one grid fill none on each other, and the two background halves (grids 2 and 3) fill none on each other. `target_cell`: used slots match donor_corner's used slots; on one receiving device the named cells are distinct and lie within 32 layers of either end of the third dimension; empty slots hold 16384.
All inputs are finite; a program needn't handle non-finite values.
Results may differ from the reference program's by a relative error of at most 0.00002.
Values sent between devices are 32-bit elements; how exact they have to be, the bound alone decides.
A program may use at most 128 MiB of HBM per device.

```python
import jax
import jax.numpy as jnp
from jax import lax

NV = 8
CX = 8
CY = 16
NZ = 128
RIM = 32
S = 32
NP = 64
NX = 128
NY = 64
CELLS = 16384
N_GRP = 4
N_GX = 16
N_GY = 4


def pair_counts(key):
    count_key = jax.random.fold_in(key, 11)
    shape = (N_GRP, NP, N_GRP, NP)
    pair_count = jax.random.randint(count_key, shape, (S + 1) // 2, S + 1)
    src_group = lax.broadcasted_iota(jnp.int32, shape, 0)
    src_device = lax.broadcasted_iota(jnp.int32, shape, 1)
    dst_group = lax.broadcasted_iota(jnp.int32, shape, 2)
    dst_device = lax.broadcasted_iota(jnp.int32, shape, 3)
    forced = (dst_group == (src_group + 2) % N_GRP) & (dst_device == src_device)
    pair_count = jnp.where(forced, S, pair_count)
    pair_count = jnp.where(src_group == dst_group, 0, pair_count)
    pair_count = jnp.where((src_group >= 2) & (dst_group >= 2), 0, pair_count)
    return (pair_count.astype(jnp.int32), forced)


def draw_donor_corner(key, part):
    pair_count, forced = pair_counts(key)
    shape = (N_GRP, NP, N_GRP, NP, S)
    key_x = jax.random.fold_in(key, 21)
    key_y = jax.random.fold_in(key, 22)
    key_z = jax.random.fold_in(key, 23)
    cell_x = jax.random.randint(key_x, shape, 0, CX - 1)
    cell_y = jax.random.randint(key_y, shape, 0, CY - 1)
    cell_z = jax.random.randint(key_z, shape, 0, NZ - 1)
    corner = (cell_x * CY + cell_y) * NZ + cell_z
    slot = lax.broadcasted_iota(jnp.int32, shape, 4)
    corner = jnp.where(slot < pair_count[..., None], corner, 0)
    highest = (CX - 2) * CY * NZ + (CY - 2) * NZ + NZ - 2
    corner = jnp.where(forced[..., None] & (slot == 0), highest, corner)
    return corner.astype(jnp.int32).reshape(N_GRP, N_GX, N_GY, N_GRP, NP, S)


def draw_target_cell(key, part):
    pair_count, forced = pair_counts(key)
    rim_count = CX * CY * 2 * RIM
    perm_keys = jax.random.split(jax.random.fold_in(key, 31), N_GRP * NP)
    orders = jax.vmap(lambda single: jax.random.permutation(single, rim_count))(perm_keys)
    chosen = orders[:, :N_GRP * NP * S].astype(jnp.int32).reshape(N_GRP, NP, N_GRP, NP, S)
    column = chosen // (2 * RIM)
    layer = chosen % (2 * RIM)
    depth = jnp.where(layer < RIM, layer, NZ - 2 * RIM + layer)
    cell = column * NZ + depth
    incoming = pair_count.transpose(2, 3, 0, 1)[..., None]
    slot = lax.broadcasted_iota(jnp.int32, chosen.shape, 4)
    cell = jnp.where(slot < incoming, cell, CELLS)
    return cell.astype(jnp.int32).reshape(N_GRP, N_GX, N_GY, N_GRP, NP, S)


def block_levels(key, extent, cuts, low, high):
    def one(dim, parts):
        draws = jax.random.uniform(jax.random.fold_in(jax.random.fold_in(key, 6), dim), (parts,), jnp.float32, low / len(cuts), high / len(cuts))
        return jnp.repeat(jnp.exp(draws), extent[dim] // parts).reshape((-1,) + (1,) * (len(extent) - dim - 1))

    gain = one(*cuts[0])
    for cut in cuts[1:]:
        gain = gain * one(*cut)
    return gain


def normal_values(rng, dims, deviation, limit, cuts=(), held_as=jnp.bfloat16):
    values = jax.random.normal(rng, dims, jnp.float32) * deviation
    if len(cuts) > 0:
        values = block_levels(rng, dims, cuts, -0.22, 0.18) * values
    return jnp.clip(values, min=-limit, max=limit).astype(held_as)


def setup_inputs(seed: int = 0) -> dict:
    keys = jax.random.split(jax.random.key(seed), 6)
    return {
        "conserved": normal_values(keys[0], (NV, N_GRP, NX, NY, NZ), 1.0, 6.0, ((1, 4), (2, 16), (3, 4)), jnp.float32),
        "velocity": jnp.clip(jax.random.uniform(keys[1], (3, N_GRP, NX, NY, NZ), jnp.float32, -0.45, 0.45) * block_levels(keys[1], (3, N_GRP, NX, NY, NZ), ((1, 4), (2, 16), (3, 4)), -0.4, 0.0), -0.45, 0.45),
        "donor_corner": draw_donor_corner(jax.random.fold_in(keys[5], 71), 0),
        "donor_fraction": jnp.clip(1.0 * jax.random.uniform(keys[3], (3, N_GRP, N_GX, N_GY, N_GRP, NP, S), jnp.float32) ** block_levels(keys[3], (3, N_GRP, N_GX, N_GY, N_GRP, NP, S), ((1, 4), (2, 16), (3, 4)), -0.2, 0.2), 0.0, 1.0),
        "target_cell": draw_target_cell(jax.random.fold_in(keys[5], 71), 0),
    }


signal_speed = 0.5
courant_number = 0.3
corner_shifts = ((0, 0, 0), (0, 0, 1), (0, 1, 0), (0, 1, 1), (1, 0, 0), (1, 0, 1), (1, 1, 0), (1, 1, 1))


def gather_corners(flat_state, corner_base, stride_x, stride_y):
    pieces = [jnp.take(flat_state, corner_base + shift[0] * stride_x + shift[1] * stride_y + shift[2], axis=1) for shift in corner_shifts]
    return jnp.stack(pieces)


def blend_corners(corners, fraction):
    total = jnp.zeros(corners.shape[1:], jnp.float32)
    for number, shift in enumerate(corner_shifts):
        weight_x = fraction[0] if shift[0] else 1.0 - fraction[0]
        weight_y = fraction[1] if shift[1] else 1.0 - fraction[1]
        weight_z = fraction[2] if shift[2] else 1.0 - fraction[2]
        weight = (weight_x * weight_y) * weight_z
        total = total + weight[None] * corners[number]
    return total


def face_pair(array, direction):
    low_index = [slice(None)] + [slice(1, -1)] * 3
    high_index = [slice(None)] + [slice(1, -1)] * 3
    low_index[direction] = slice(0, -1)
    high_index[direction] = slice(1, None)
    return array[tuple(low_index)], array[tuple(high_index)]


def step_diff(array, direction):
    lower = [slice(None)] * 4
    upper = [slice(None)] * 4
    lower[direction] = slice(0, -1)
    upper[direction] = slice(1, None)
    return array[tuple(upper)] - array[tuple(lower)]


def central(field, direction):
    lower = [slice(1, -1)] * 3
    upper = [slice(1, -1)] * 3
    lower[direction] = slice(0, -2)
    upper[direction] = slice(2, None)
    return 0.5 * (field[tuple(upper)] - field[tuple(lower)])


def advance(conserved, speeds):
    hydro = conserved[:5]
    magnetic = conserved[5:]
    change = jnp.zeros(hydro[:, 1:-1, 1:-1, 1:-1].shape, jnp.float32)
    for direction in (1, 2, 3):
        state_low, state_high = face_pair(hydro, direction)
        speed_low, speed_high = face_pair(speeds[direction - 1:direction], direction)
        wave_low = jnp.minimum(jnp.minimum(speed_low, speed_high) - signal_speed, 0.0)
        wave_high = jnp.maximum(jnp.maximum(speed_low, speed_high) + signal_speed, 0.0)
        flux = (wave_high * speed_low * state_low - wave_low * speed_high * state_high + wave_low * wave_high * (state_high - state_low)) / (wave_high - wave_low)
        change = change + step_diff(flux, direction)
    hydro_next = hydro[:, 1:-1, 1:-1, 1:-1] - courant_number * change
    elec_x = -(speeds[1] * magnetic[2] - speeds[2] * magnetic[1])
    elec_y = -(speeds[2] * magnetic[0] - speeds[0] * magnetic[2])
    elec_z = -(speeds[0] * magnetic[1] - speeds[1] * magnetic[0])
    curl_x = central(elec_z, 1) - central(elec_y, 2)
    curl_y = central(elec_x, 2) - central(elec_z, 0)
    curl_z = central(elec_y, 0) - central(elec_x, 1)
    magnetic_next = magnetic[:, 1:-1, 1:-1, 1:-1] - courant_number * jnp.stack([curl_x, curl_y, curl_z])
    return jnp.concatenate([hydro_next, magnetic_next], axis=0)


def reference(conserved, velocity, donor_corner, donor_fraction, target_cell):
    devices = N_GRP * NP
    blocks = conserved.reshape(NV, N_GRP, N_GX, CX, N_GY, CY, NZ).transpose(1, 2, 4, 0, 3, 5, 6).reshape(devices, NV, CELLS)
    bases = donor_corner.reshape(devices, N_GRP, NP, S)
    fractions = donor_fraction.reshape(3, devices, N_GRP, NP, S).transpose(1, 0, 2, 3, 4)

    def donate(packed):
        return blend_corners(gather_corners(packed[0], packed[1], CY * NZ, NZ), packed[2])

    sent = lax.map(donate, (blocks, bases, fractions))
    received = sent.reshape(devices, NV, devices, S).transpose(2, 1, 0, 3).reshape(devices, NV, devices * S)
    targets = target_cell.reshape(devices, devices * S)

    def place(packed):
        return packed[0].at[:, packed[2]].set(packed[1], mode="drop")

    filled = lax.map(place, (blocks, received, targets))
    grid = filled.reshape(N_GRP, N_GX, N_GY, NV, CX, CY, NZ).transpose(0, 3, 1, 4, 2, 5, 6).reshape(N_GRP, NV, NX, NY, NZ)
    speeds = velocity.transpose(1, 0, 2, 3, 4)
    widths = ((0, 0), (1, 1), (1, 1), (1, 1))

    def update(packed):
        return advance(jnp.pad(packed[0], widths), jnp.pad(packed[1], widths))

    result = lax.map(update, (grid, speeds))
    return result.transpose(1, 0, 2, 3, 4)
```

```python
import jax
import jax.numpy as jnp
from jax import lax
from jax.experimental import pallas as pl
from jax.experimental.pallas import tpu as pltpu
from jax.sharding import PartitionSpec as P

signal_speed = 0.5
courant_number = 0.3
f32 = jnp.float32
bf16 = jnp.bfloat16
MESH = pl.DeviceIdType.MESH
VMEM = pl.BlockSpec(memory_space=pltpu.VMEM)


def halves(x):
    head = x.astype(bf16)
    return head, (x - head.astype(f32)).astype(bf16)


def grid_step(k):
    return 1 + lax.rem(k + 1, 3)


def packed_rows(block):
    return jnp.concatenate([block[0:8], block[16:24], block[8:16], block[24:32]], axis=1)


def gather_kernel(state_ref, corner_ref, frac_ref, out_ref, lhs, ints, floats, prod, turned):
    g = lax.axis_index("grp")
    head, rest = halves(state_ref[...])
    lhs[:, 0:128] = head
    lhs[:, 128:256] = rest

    @pl.loop(0, 3)
    def _(k):
        h = lax.rem(g + grid_step(k), 4)
        ints[...] = packed_rows(corner_ref[h])
        for d in range(3):
            floats[d] = packed_rows(frac_ref[d, h])

        @pl.loop(0, 8)
        def _(rr):
            base = ints[pl.ds(rr, 1), :]
            fx = floats[0, pl.ds(rr, 1), :]
            fy = floats[1, pl.ds(rr, 1), :]
            fz = floats[2, pl.ds(rr, 1), :]
            cz = base & 127
            cy = (base >> 7) & 15
            cx = base >> 11
            iz = lax.broadcasted_iota(jnp.int32, (128, 256), 0)
            wz = jnp.where(iz == cz, 1.0 - fz, jnp.where(iz == cz + 1, fz, 0.0))
            z_head, z_rest = halves(wz)
            both = lhs[...]
            prod[...] = jnp.dot(
                both, jnp.concatenate([z_head, z_head], axis=0), preferred_element_type=f32
            ) + jnp.dot(both, jnp.concatenate([z_rest, z_rest], axis=0), preferred_element_type=f32)
            iy = lax.broadcasted_iota(jnp.int32, (16, 256), 0)
            wy = jnp.where(iy == cy, 1.0 - fy, jnp.where(iy == cy + 1, fy, 0.0))
            wx = [jnp.where(cx == x, 1.0 - fx, jnp.where(cx + 1 == x, fx, 0.0)) for x in range(8)]
            rows = []
            for v in range(8):
                total = prod[v * 128 : v * 128 + 16, :] * wx[0]
                for x in range(1, 8):
                    start = v * 128 + x * 16
                    total = total + prod[start : start + 16, :] * wx[x]
                rows.append(jnp.sum(total * wy, axis=0, keepdims=True))
            values = jnp.concatenate(rows, axis=0)
            turned[pl.ds(pl.multiple_of(rr * 8, 8), 8), :] = values[:, 0:128]
            turned[pl.ds(pl.multiple_of(64 + rr * 8, 8), 8), :] = values[:, 128:256]

        out_ref[k] = turned[...].T


def gather(state, corner, frac):
    return pl.pallas_call(
        gather_kernel,
        out_shape=jax.ShapeDtypeStruct((3, 128, 128), f32),
        in_specs=[VMEM] * 3,
        out_specs=VMEM,
        scratch_shapes=[
            pltpu.VMEM((1024, 256), bf16),
            pltpu.VMEM((8, 256), jnp.int32),
            pltpu.VMEM((3, 8, 256), f32),
            pltpu.VMEM((1024, 256), f32),
            pltpu.VMEM((128, 128), f32),
        ],
        name="gather",
    )(state, corner, frac)


def side_copies(face_x, face_y, land_x, land_y, send, recv):
    i, j = lax.axis_index("gx"), lax.axis_index("gy")
    up_x, down_x = lax.rem(i + 1, 16), lax.rem(i + 15, 16)
    up_y, down_y = lax.rem(j + 1, 4), lax.rem(j + 3, 4)
    copies = []
    for n, (src, dst, where) in enumerate(
        (
            (face_x.at[:, 7], land_x.at[0], {"gx": up_x}),
            (face_x.at[:, 0], land_x.at[1], {"gx": down_x}),
            (face_y.at[1], land_y.at[0], {"gy": up_y}),
            (face_y.at[0], land_y.at[1], {"gy": down_y}),
        )
    ):
        copies.append(
            pltpu.make_async_remote_copy(
                src_ref=src,
                dst_ref=dst,
                send_sem=send.at[n],
                recv_sem=recv.at[n],
                device_id=where,
                device_id_type=MESH,
            )
        )
    return copies


def greet_sides(barrier):
    i, j = lax.axis_index("gx"), lax.axis_index("gy")
    for where in (
        {"gx": lax.rem(i + 1, 16)},
        {"gx": lax.rem(i + 15, 16)},
        {"gy": lax.rem(j + 1, 4)},
        {"gy": lax.rem(j + 3, 4)},
    ):
        pl.semaphore_signal(barrier, inc=1, device_id=where, device_id_type=MESH)


def exchange_kernel(
    out_vals, vel_ref, in_vals, vel_x, vel_y, face_y, send, recv, side_send, side_recv
):
    g, i, j = lax.axis_index("grp"), lax.axis_index("gx"), lax.axis_index("gy")
    me = i * 4 + j
    barrier = pltpu.get_barrier_semaphore()

    @pl.loop(0, 192)
    def _(n):
        k, q = n // 64, lax.rem(n, 64)
        where = {"grp": lax.rem(g + grid_step(k), 4), "gx": q // 4, "gy": lax.rem(q, 4)}
        pl.semaphore_signal(barrier, inc=1, device_id=where, device_id_type=MESH)

    greet_sides(barrier)
    face_y[0] = vel_ref[:, :, 0, :]
    face_y[1] = vel_ref[:, :, 15, :]
    pl.semaphore_wait(barrier, 196)

    @pl.loop(0, 192)
    def _(n):
        k, q = n // 64, lax.rem(n, 64)
        where = {"grp": lax.rem(g + grid_step(k), 4), "gx": q // 4, "gy": lax.rem(q, 4)}
        pltpu.make_async_remote_copy(
            src_ref=out_vals.at[k, :, q],
            dst_ref=in_vals.at[k, :, me],
            send_sem=send,
            recv_sem=recv,
            device_id=where,
            device_id_type=MESH,
        ).start()

    sides = side_copies(vel_ref, face_y, vel_x, vel_y, side_send, side_recv)
    for copy in sides:
        copy.start()
    whole = pltpu.make_async_remote_copy(
        src_ref=out_vals,
        dst_ref=in_vals,
        send_sem=send,
        recv_sem=recv,
        device_id={"gx": lax.rem(i + 1, 16)},
        device_id_type=MESH,
    )
    whole.wait_send()
    whole.wait_recv()
    for copy in sides:
        copy.wait()


def exchange(out_vals, velocity):
    return pl.pallas_call(
        exchange_kernel,
        out_shape=(
            jax.ShapeDtypeStruct((3, 2, 64, 1, 128), f32),
            jax.ShapeDtypeStruct((2, 3, 16, 128), f32),
            jax.ShapeDtypeStruct((2, 3, 8, 128), f32),
        ),
        in_specs=[VMEM] * 2,
        out_specs=(VMEM,) * 3,
        scratch_shapes=[
            pltpu.VMEM((2, 3, 8, 128), f32),
            pltpu.SemaphoreType.DMA,
            pltpu.SemaphoreType.DMA,
            pltpu.SemaphoreType.DMA((4,)),
            pltpu.SemaphoreType.DMA((4,)),
        ],
        compiler_params=pltpu.CompilerParams(collective_id=0, has_side_effects=True),
        name="exchange",
    )(out_vals, velocity)


def place_kernel(
    vals_ref, target_ref, state_ref, filled, land_x, land_y, lhs, rhs, acc, ints, turned, face_y,
    send, recv,
):
    g = lax.axis_index("grp")
    barrier = pltpu.get_barrier_semaphore()
    greet_sides(barrier)
    acc[...] = jnp.zeros_like(acc)

    @pl.loop(0, 3)
    def _(k):
        source = lax.rem(g + 4 - grid_step(k), 4)
        ints[...] = packed_rows(target_ref[source])
        turned[...] = vals_ref[k].T

        @pl.loop(0, 8)
        def _(rr):
            cell = ints[pl.ds(rr, 1), :]
            column = cell >> 7
            row = column & 31
            lane = ((column >> 6) << 7) + (((cell & 127) + ((column & 32) << 1)) & 127)
            values = jnp.concatenate(
                [
                    turned[pl.ds(pl.multiple_of(rr * 8, 8), 8), :],
                    turned[pl.ds(pl.multiple_of(64 + rr * 8, 8), 8), :],
                ],
                axis=1,
            )
            head = values.astype(bf16).astype(f32)
            rest = values - head
            hit = lax.broadcasted_iota(jnp.int32, (32, 256), 0) == row
            at = pl.ds(pl.multiple_of(rr * 256, 256), 256)
            for v in range(8):
                lhs[v * 32 : v * 32 + 32, at] = jnp.where(hit, head[v : v + 1, :], 0.0).astype(bf16)
                lhs[256 + v * 32 : 288 + v * 32, at] = jnp.where(
                    hit, rest[v : v + 1, :], 0.0
                ).astype(bf16)
            lhs[512:544, at] = jnp.where(hit, 1.0, 0.0).astype(bf16)
            il = lax.broadcasted_iota(jnp.int32, (256, 256), 0)
            rhs[:, at] = jnp.where(il == lane, 1.0, 0.0).astype(bf16)

        acc[...] += lax.dot_general(
            lhs[...], rhs[...], (((1,), (1,)), ((), ())), preferred_element_type=f32
        )

    spot = lax.broadcasted_iota(jnp.int32, (32, 128), 1)
    rim = (spot < 32) | (spot >= 96)
    for pair in range(2):
        span = slice(pair * 128, pair * 128 + 128)
        count = acc[512:544, span]
        for b in range(2):
            seen = pltpu.roll(count, 64, 1) if b else count
            hit = rim & (seen > 0.5)
            x = 4 * pair + 2 * b
            for v in range(8):
                new = acc[v * 32 : v * 32 + 32, span] + acc[256 + v * 32 : 288 + v * 32, span]
                if b:
                    new = pltpu.roll(new, 64, 1)
                old = state_ref[v, x : x + 2].reshape(32, 128)
                filled[v, x : x + 2] = jnp.where(hit, new, old).reshape(2, 16, 128)
    face_y[0] = filled[:, :, 0, :]
    face_y[1] = filled[:, :, 15, :]
    pl.semaphore_wait(barrier, 4)
    sides = side_copies(filled, face_y, land_x, land_y, send, recv)
    for copy in sides:
        copy.start()
    for copy in sides:
        copy.wait()


def place(vals, target, state):
    return pl.pallas_call(
        place_kernel,
        out_shape=(
            jax.ShapeDtypeStruct((8, 8, 16, 128), f32),
            jax.ShapeDtypeStruct((2, 8, 16, 128), f32),
            jax.ShapeDtypeStruct((2, 8, 8, 128), f32),
        ),
        in_specs=[VMEM] * 3,
        out_specs=(VMEM,) * 3,
        scratch_shapes=[
            pltpu.VMEM((544, 2048), bf16),
            pltpu.VMEM((256, 2048), bf16),
            pltpu.VMEM((544, 256), f32),
            pltpu.VMEM((8, 256), jnp.int32),
            pltpu.VMEM((128, 128), f32),
            pltpu.VMEM((2, 8, 8, 128), f32),
            pltpu.SemaphoreType.DMA((4,)),
            pltpu.SemaphoreType.DMA((4,)),
        ],
        compiler_params=pltpu.CompilerParams(collective_id=1, has_side_effects=True),
        name="place",
    )(vals, target, state)


def face_weights(low, high):
    wave_low = jnp.minimum(jnp.minimum(low, high) - signal_speed, 0.0)
    wave_high = jnp.maximum(jnp.maximum(low, high) + signal_speed, 0.0)
    scale = courant_number / (wave_high - wave_low)
    return (
        wave_high * (low - wave_low) * scale,
        wave_low * (wave_high - high) * scale,
    )


def step_kernel(u_ref, vel_ref, ux_ref, uy_ref, vx_ref, vy_ref, out_ref):
    i, j = lax.axis_index("gx"), lax.axis_index("gy")
    lane = lax.broadcasted_iota(jnp.int32, (16, 128), 1)
    line = lax.broadcasted_iota(jnp.int32, (16, 128), 0)
    keep_low_x, keep_high_x = i > 0, i < 15
    keep_low_y, keep_high_y = j > 0, j < 3

    def plane(ref, side, v, x):
        if x < 0:
            return jnp.where(keep_low_x, side[0, v], 0.0)
        if x > 7:
            return jnp.where(keep_high_x, side[1, v], 0.0)
        return ref[v, x]

    def row(side, which, v, x):
        keep = keep_high_y if which else keep_low_y
        return jnp.where(keep, side[which, v, x : x + 1, :], 0.0)

    def prev_z(a):
        return jnp.where(lane == 0, 0.0, pltpu.roll(a, 1, 1))

    def next_z(a):
        return jnp.where(lane == 127, 0.0, pltpu.roll(a, 127, 1))

    def prev_y(a, low):
        return jnp.where(line == 0, low, pltpu.roll(a, 1, 0))

    def next_y(a, high):
        return jnp.where(line == 15, high, pltpu.roll(a, 15, 0))

    def elec(b, v):
        return (v[2] * b[1] - v[1] * b[2], v[0] * b[2] - v[2] * b[0], v[1] * b[0] - v[0] * b[1])

    speed = [[plane(vel_ref, vx_ref, d, x) for d in range(3)] for x in range(-1, 9)]
    weights_x = [face_weights(speed[x][0], speed[x + 1][0]) for x in range(9)]
    fields = [
        elec([plane(u_ref, ux_ref, 5 + d, x) for d in range(3)], speed[x + 1]) for x in range(-1, 9)
    ]
    flux_low = [
        weights_x[0][0] * plane(u_ref, ux_ref, v, -1) + weights_x[0][1] * u_ref[v, 0]
        for v in range(5)
    ]
    for x in range(8):
        here = speed[x + 1]
        low_v = [row(vy_ref, 0, d, x) for d in range(3)]
        high_v = [row(vy_ref, 1, d, x) for d in range(3)]
        y_low = face_weights(prev_y(here[1], low_v[1]), here[1])
        y_high = face_weights(here[1], next_y(here[1], high_v[1]))
        z_low = face_weights(prev_z(here[2]), here[2])
        z_high = face_weights(here[2], next_z(here[2]))
        centre = (
            1.0
            + y_low[1] - y_high[0]
            + z_low[1] - z_high[0]
        )
        for v in range(5):
            u = u_ref[v, x]
            flux_high = weights_x[x + 1][0] * u + weights_x[x + 1][1] * plane(
                u_ref, ux_ref, v, x + 1
            )
            new = centre * u - (flux_high - flux_low[v])
            flux_low[v] = flux_high
            new = new + y_low[0] * prev_y(u, row(uy_ref, 0, v, x))
            new = new - y_high[1] * next_y(u, row(uy_ref, 1, v, x))
            new = new + z_low[0] * prev_z(u)
            new = new - z_high[1] * next_z(u)
            out_ref[v, x] = new
        below, e, above = fields[x], fields[x + 1], fields[x + 2]
        e_low = elec([row(uy_ref, 0, 5 + d, x) for d in range(3)], low_v)
        e_high = elec([row(uy_ref, 1, 5 + d, x) for d in range(3)], high_v)

        def along_y(d):
            return next_y(e[d], e_high[d]) - prev_y(e[d], e_low[d])

        def along_z(d):
            return next_z(e[d]) - prev_z(e[d])

        def along_x(d):
            return above[d] - below[d]

        half = 0.5 * courant_number
        out_ref[5, x] = u_ref[5, x] - half * (along_y(2) - along_z(1))
        out_ref[6, x] = u_ref[6, x] - half * (along_z(0) - along_x(2))
        out_ref[7, x] = u_ref[7, x] - half * (along_x(1) - along_y(0))


def step(u, vel, ux, uy, vx, vy):
    return pl.pallas_call(
        step_kernel,
        out_shape=jax.ShapeDtypeStruct((8, 8, 16, 128), f32),
        in_specs=[VMEM] * 6,
        out_specs=VMEM,
        name="step",
    )(u, vel, ux, uy, vx, vy)


def per_device(conserved, velocity, donor_corner, donor_fraction, target_cell):
    state = conserved[:, 0]
    speeds = velocity[:, 0]
    corner = donor_corner[0, 0, 0].transpose(0, 2, 1)
    frac = donor_fraction[:, 0, 0, 0].transpose(0, 1, 3, 2)
    target = target_cell[0, 0, 0].transpose(0, 2, 1)
    sent = gather(state.reshape(1024, 128), corner, frac)
    came, vel_x, vel_y = exchange(sent.reshape(3, 2, 64, 1, 128), speeds)
    filled, u_x, u_y = place(came.reshape(3, 128, 128), target, state)
    return step(filled, speeds, u_x, u_y, vel_x, vel_y)[:, None]


def solution(mesh):
    return jax.shard_map(
        per_device,
        mesh=mesh,
        in_specs=(
            P(None, "grp", "gx", "gy", None),
            P(None, "grp", "gx", "gy", None),
            P("grp", "gx", "gy", None, None, None),
            P(None, "grp", "gx", "gy", None, None, None),
            P("grp", "gx", "gy", None, None, None),
        ),
        out_specs=P(None, "grp", "gx", "gy", None),
        check_vma=False,
    )
```

```python
import jax
import jax.numpy as jnp
from jax import lax
from jax.experimental import pallas as pl
from jax.experimental.pallas import tpu as pltpu
from jax.sharding import PartitionSpec as P

signal_speed = 0.5
courant_number = 0.3
f32 = jnp.float32
bf16 = jnp.bfloat16
MESH = pl.DeviceIdType.MESH
VMEM = pl.BlockSpec(memory_space=pltpu.VMEM)


def halves(x):
    head = x.astype(bf16)
    return head, (x - head.astype(f32)).astype(bf16)


def grid_step(k):
    return 1 + lax.rem(k + 1, 3)


def packed_rows(block):
    return jnp.concatenate([block[0:8], block[16:24], block[8:16], block[24:32]], axis=1)


def neighbours():
    i, j = lax.axis_index("gx"), lax.axis_index("gy")
    return (
        {"gx": lax.rem(i + 1, 16)},
        {"gx": lax.rem(i + 15, 16)},
        {"gy": lax.rem(j + 1, 4)},
        {"gy": lax.rem(j + 3, 4)},
    )


def side_copies(face_x, face_y, land_x, land_y, send, recv):
    pairs = (
        (face_x.at[:, 7], land_x.at[0]),
        (face_x.at[:, 0], land_x.at[1]),
        (face_y.at[1], land_y.at[0]),
        (face_y.at[0], land_y.at[1]),
    )
    return [
        remote(src, dst, send.at[n], recv.at[n], where)
        for n, ((src, dst), where) in enumerate(zip(pairs, neighbours()))
    ]


def remote(src, dst, send, recv, where):
    return pltpu.make_async_remote_copy(
        src_ref=src,
        dst_ref=dst,
        send_sem=send,
        recv_sem=recv,
        device_id=where,
        device_id_type=MESH,
    )


def interpolate(rr, lhs, ints, floats, prod, turned):
    base = ints[pl.ds(rr, 1), :]
    fx = floats[0, pl.ds(rr, 1), :]
    fy = floats[1, pl.ds(rr, 1), :]
    fz = floats[2, pl.ds(rr, 1), :]
    cz = base & 127
    cy = (base >> 7) & 15
    cx = base >> 11
    iz = lax.broadcasted_iota(jnp.int32, (128, 256), 0)
    wz = jnp.where(iz == cz, 1.0 - fz, jnp.where(iz == cz + 1, fz, 0.0))
    z_head, z_rest = halves(wz)
    both = lhs[...]
    prod[...] = jnp.dot(
        both, jnp.concatenate([z_head, z_head], axis=0), preferred_element_type=f32
    ) + jnp.dot(both, jnp.concatenate([z_rest, z_rest], axis=0), preferred_element_type=f32)
    iy = lax.broadcasted_iota(jnp.int32, (16, 256), 0)
    wy = jnp.where(iy == cy, 1.0 - fy, jnp.where(iy == cy + 1, fy, 0.0))
    wx = [jnp.where(cx == x, 1.0 - fx, jnp.where(cx + 1 == x, fx, 0.0)) for x in range(8)]
    rows = []
    for v in range(8):
        total = prod[v * 128 : v * 128 + 16, :] * wx[0]
        for x in range(1, 8):
            start = v * 128 + x * 16
            total = total + prod[start : start + 16, :] * wx[x]
        rows.append(jnp.sum(total * wy, axis=0, keepdims=True))
    values = jnp.concatenate(rows, axis=0)
    turned[pl.ds(pl.multiple_of(rr * 8, 8), 8), :] = values[:, 0:128]
    turned[pl.ds(pl.multiple_of(64 + rr * 8, 8), 8), :] = values[:, 128:256]


def spots(ints, rr):
    cell = ints[pl.ds(rr, 1), :]
    column = cell >> 7
    lane = ((column >> 6) << 7) + (((cell & 127) + ((column & 32) << 1)) & 127)
    return column & 31, lane


def section_kernel(
    state_ref, vel_ref, corner_ref, frac_ref, target_ref,
    filled, u_x, u_y, v_x, v_y,
    lhs, ints, floats, prods, turned, first, second, third, put_rows, put_lanes, acc, cells,
    face_u, face_v,
    y_send, y_recv, d_send, d_recv, v_send, v_recv, u_send, u_recv,
):
    g, i, j = lax.axis_index("grp"), lax.axis_index("gx"), lax.axis_index("gy")
    barrier = pltpu.get_barrier_semaphore()

    @pl.loop(0, 48)
    def _(n):
        where = {"grp": lax.rem(g + 1 + n // 16, 4), "gx": lax.rem(n, 16)}
        pl.semaphore_signal(barrier, inc=1, device_id=where, device_id_type=MESH)

    for d in range(1, 4):
        where = {"gy": lax.rem(j + d, 4)}
        pl.semaphore_signal(barrier, inc=1, device_id=where, device_id_type=MESH)
    for where in neighbours()[:2]:
        pl.semaphore_signal(barrier, inc=1, device_id=where, device_id_type=MESH)

    head, rest = halves(state_ref[...].reshape(1024, 128))
    lhs[:, 0:128] = head
    lhs[:, 128:256] = rest
    face_v[0] = vel_ref[:, :, 0, :]
    face_v[1] = vel_ref[:, :, 15, :]
    v_sides = side_copies(vel_ref, face_v, v_x, v_y, v_send, v_recv)

    def onward(k):
        some = first.at[0, :, :, 0:3]
        remote(some, second.at[k, :, :, 0:3], y_send, y_recv.at[k], {"gx": i}).wait_recv()

        @pl.loop(0, 16)
        def _(to):
            where = {"grp": lax.rem(g + grid_step(k), 4), "gx": to}
            remote(second.at[k, :, to], third.at[k, :, i], d_send, d_recv.at[k], where).start()

    @pl.loop(0, 3)
    def _(k):
        h = lax.rem(g + grid_step(k), 4)
        ints[...] = packed_rows(corner_ref[h])
        for d in range(3):
            floats[d] = packed_rows(frac_ref[d, h])

        @pl.loop(0, 8 // len(prods))
        def _(step):
            for n, prod in enumerate(prods):
                interpolate(step * len(prods) + n, lhs, ints, floats, prod, turned)

        first[k] = turned[...].T.reshape(2, 16, 4, 1, 128)
        second[k, :, :, j] = first[k, :, :, j]

        @pl.when(k == 0)
        def _():
            pl.semaphore_wait(barrier, 53)

        for d in range(1, 4):
            to = lax.rem(j + d, 4)
            remote(
                first.at[k, :, :, to], second.at[k, :, :, j], y_send, y_recv.at[k], {"gy": to}
            ).start()

        @pl.when(k == 0)
        def _():
            for copy in v_sides:
                copy.start()

        @pl.when(k > 0)
        def _():
            onward(k - 1)

    @pl.loop(0, 3)
    def _(k):
        cells[k] = packed_rows(target_ref[lax.rem(g + 4 - grid_step(k), 4)])

    onward(2)

    @pl.loop(0, 24)
    def _(n):
        k, rr = n // 8, lax.rem(n, 8)
        _, lane = spots(cells.at[k], rr)
        il = lax.broadcasted_iota(jnp.int32, (256, 256), 0)
        put_lanes[:, pl.ds(pl.multiple_of(n * 256, 256), 256)] = jnp.where(
            il == lane, 1.0, 0.0
        ).astype(bf16)

    acc[...] = jnp.zeros_like(acc)

    @pl.loop(0, 3)
    def _(k):
        remote(second.at[k], third.at[k], d_send, d_recv.at[k], {"gx": i}).wait_recv()
        turned[...] = third[k].reshape(128, 128).T

        @pl.loop(0, 8)
        def _(rr):
            row, _ = spots(cells.at[k], rr)
            values = jnp.concatenate(
                [
                    turned[pl.ds(pl.multiple_of(rr * 8, 8), 8), :],
                    turned[pl.ds(pl.multiple_of(64 + rr * 8, 8), 8), :],
                ],
                axis=1,
            )
            head = values.astype(bf16).astype(f32)
            rest = values - head
            hit = lax.broadcasted_iota(jnp.int32, (32, 256), 0) == row
            at = pl.ds(pl.multiple_of(rr * 256, 256), 256)
            for v in range(8):
                put_rows[v * 32 : v * 32 + 32, at] = jnp.where(hit, head[v : v + 1, :], 0.0).astype(
                    bf16
                )
                put_rows[256 + v * 32 : 288 + v * 32, at] = jnp.where(
                    hit, rest[v : v + 1, :], 0.0
                ).astype(bf16)
            put_rows[512:544, at] = jnp.where(hit, 1.0, 0.0).astype(bf16)

        acc[...] += lax.dot_general(
            put_rows[...],
            put_lanes[:, pl.ds(pl.multiple_of(k * 2048, 2048), 2048)],
            (((1,), (1,)), ((), ())),
            preferred_element_type=f32,
        )

    spot = lax.broadcasted_iota(jnp.int32, (32, 128), 1)
    rim = (spot < 32) | (spot >= 96)
    for pair in range(2):
        span = slice(pair * 128, pair * 128 + 128)
        count = acc[512:544, span]
        for b in range(2):
            seen = pltpu.roll(count, 64, 1) if b else count
            hit = rim & (seen > 0.5)
            x = 4 * pair + 2 * b
            for v in range(8):
                new = acc[v * 32 : v * 32 + 32, span] + acc[256 + v * 32 : 288 + v * 32, span]
                if b:
                    new = pltpu.roll(new, 64, 1)
                old = state_ref[v, x : x + 2].reshape(32, 128)
                filled[v, x : x + 2] = jnp.where(hit, new, old).reshape(2, 16, 128)
    face_u[0] = filled[:, :, 0, :]
    face_u[1] = filled[:, :, 15, :]
    u_sides = side_copies(filled, face_u, u_x, u_y, u_send, u_recv)
    for copy in u_sides:
        copy.start()
    for copy in v_sides + u_sides:
        copy.wait()
    remote(first.at[:, :, :, 0:3], second.at[:, :, :, 0:3], y_send, y_recv.at[0], {"gx": i}).wait_send()
    remote(second, third, d_send, d_recv.at[0], {"gx": i}).wait_send()


UNROLL = 2


def section(state, velocity, corner, frac, target):
    dma = pltpu.SemaphoreType.DMA
    chunk = pltpu.VMEM((3, 2, 16, 4, 1, 128), f32)
    return pl.pallas_call(
        section_kernel,
        out_shape=(
            jax.ShapeDtypeStruct((8, 8, 16, 128), f32),
            jax.ShapeDtypeStruct((2, 8, 16, 128), f32),
            jax.ShapeDtypeStruct((2, 8, 8, 128), f32),
            jax.ShapeDtypeStruct((2, 3, 16, 128), f32),
            jax.ShapeDtypeStruct((2, 3, 8, 128), f32),
        ),
        in_specs=[VMEM] * 5,
        out_specs=(VMEM,) * 5,
        scratch_shapes=[
            pltpu.VMEM((1024, 256), bf16),
            pltpu.VMEM((8, 256), jnp.int32),
            pltpu.VMEM((3, 8, 256), f32),
            [pltpu.VMEM((1024, 256), f32) for _ in range(UNROLL)],
            pltpu.VMEM((128, 128), f32),
            chunk,
            chunk,
            chunk,
            pltpu.VMEM((544, 2048), bf16),
            pltpu.VMEM((256, 6144), bf16),
            pltpu.VMEM((544, 256), f32),
            pltpu.VMEM((3, 8, 256), jnp.int32),
            pltpu.VMEM((2, 8, 8, 128), f32),
            pltpu.VMEM((2, 3, 8, 128), f32),
            dma,
            dma((3,)),
            dma,
            dma((3,)),
            dma((4,)),
            dma((4,)),
            dma((4,)),
            dma((4,)),
        ],
        compiler_params=pltpu.CompilerParams(collective_id=0, has_side_effects=True),
        name="section",
    )(state, velocity, corner, frac, target)


def face_weights(low, high):
    wave_low = jnp.minimum(jnp.minimum(low, high) - signal_speed, 0.0)
    wave_high = jnp.maximum(jnp.maximum(low, high) + signal_speed, 0.0)
    scale = courant_number / (wave_high - wave_low)
    return (
        wave_high * (low - wave_low) * scale,
        wave_low * (wave_high - high) * scale,
    )


def step_kernel(u_ref, vel_ref, ux_ref, uy_ref, vx_ref, vy_ref, out_ref):
    i, j = lax.axis_index("gx"), lax.axis_index("gy")
    lane = lax.broadcasted_iota(jnp.int32, (16, 128), 1)
    line = lax.broadcasted_iota(jnp.int32, (16, 128), 0)
    keep_low_x, keep_high_x = i > 0, i < 15
    keep_low_y, keep_high_y = j > 0, j < 3

    def plane(ref, side, v, x):
        if x < 0:
            return jnp.where(keep_low_x, side[0, v], 0.0)
        if x > 7:
            return jnp.where(keep_high_x, side[1, v], 0.0)
        return ref[v, x]

    def row(side, which, v, x):
        keep = keep_high_y if which else keep_low_y
        return jnp.where(keep, side[which, v, x : x + 1, :], 0.0)

    def prev_z(a):
        return jnp.where(lane == 0, 0.0, pltpu.roll(a, 1, 1))

    def next_z(a):
        return jnp.where(lane == 127, 0.0, pltpu.roll(a, 127, 1))

    def prev_y(a, low):
        return jnp.where(line == 0, low, pltpu.roll(a, 1, 0))

    def next_y(a, high):
        return jnp.where(line == 15, high, pltpu.roll(a, 15, 0))

    def elec(b, v):
        return (v[2] * b[1] - v[1] * b[2], v[0] * b[2] - v[2] * b[0], v[1] * b[0] - v[0] * b[1])

    speed = [[plane(vel_ref, vx_ref, d, x) for d in range(3)] for x in range(-1, 9)]
    weights_x = [face_weights(speed[x][0], speed[x + 1][0]) for x in range(9)]
    fields = [
        elec([plane(u_ref, ux_ref, 5 + d, x) for d in range(3)], speed[x + 1]) for x in range(-1, 9)
    ]
    flux_low = [
        weights_x[0][0] * plane(u_ref, ux_ref, v, -1) + weights_x[0][1] * u_ref[v, 0]
        for v in range(5)
    ]
    for x in range(8):
        here = speed[x + 1]
        low_v = [row(vy_ref, 0, d, x) for d in range(3)]
        high_v = [row(vy_ref, 1, d, x) for d in range(3)]
        y_low = face_weights(prev_y(here[1], low_v[1]), here[1])
        y_high = face_weights(here[1], next_y(here[1], high_v[1]))
        z_low = face_weights(prev_z(here[2]), here[2])
        z_high = face_weights(here[2], next_z(here[2]))
        centre = (
            1.0
            + y_low[1] - y_high[0]
            + z_low[1] - z_high[0]
        )
        for v in range(5):
            u = u_ref[v, x]
            flux_high = weights_x[x + 1][0] * u + weights_x[x + 1][1] * plane(
                u_ref, ux_ref, v, x + 1
            )
            new = centre * u - (flux_high - flux_low[v])
            flux_low[v] = flux_high
            new = new + y_low[0] * prev_y(u, row(uy_ref, 0, v, x))
            new = new - y_high[1] * next_y(u, row(uy_ref, 1, v, x))
            new = new + z_low[0] * prev_z(u)
            new = new - z_high[1] * next_z(u)
            out_ref[v, x] = new
        below, e, above = fields[x], fields[x + 1], fields[x + 2]
        e_low = elec([row(uy_ref, 0, 5 + d, x) for d in range(3)], low_v)
        e_high = elec([row(uy_ref, 1, 5 + d, x) for d in range(3)], high_v)

        def along_y(d):
            return next_y(e[d], e_high[d]) - prev_y(e[d], e_low[d])

        def along_z(d):
            return next_z(e[d]) - prev_z(e[d])

        def along_x(d):
            return above[d] - below[d]

        half = 0.5 * courant_number
        out_ref[5, x] = u_ref[5, x] - half * (along_y(2) - along_z(1))
        out_ref[6, x] = u_ref[6, x] - half * (along_z(0) - along_x(2))
        out_ref[7, x] = u_ref[7, x] - half * (along_x(1) - along_y(0))


def step(u, vel, ux, uy, vx, vy):
    return pl.pallas_call(
        step_kernel,
        out_shape=jax.ShapeDtypeStruct((8, 8, 16, 128), f32),
        in_specs=[VMEM] * 6,
        out_specs=VMEM,
        name="step",
    )(u, vel, ux, uy, vx, vy)


def per_device(conserved, velocity, donor_corner, donor_fraction, target_cell):
    state = conserved[:, 0]
    speeds = velocity[:, 0]
    corner = donor_corner[0, 0, 0].transpose(0, 2, 1)
    frac = donor_fraction[:, 0, 0, 0].transpose(0, 1, 3, 2)
    target = target_cell[0, 0, 0].transpose(0, 2, 1)
    filled, u_x, u_y, v_x, v_y = section(state, speeds, corner, frac, target)
    return step(filled, speeds, u_x, u_y, v_x, v_y)[:, None]


def solution(mesh):
    return jax.shard_map(
        per_device,
        mesh=mesh,
        in_specs=(
            P(None, "grp", "gx", "gy", None),
            P(None, "grp", "gx", "gy", None),
            P("grp", "gx", "gy", None, None, None),
            P(None, "grp", "gx", "gy", None, None, None),
            P("grp", "gx", "gy", None, None, None),
        ),
        out_specs=P(None, "grp", "gx", "gy", None),
        check_vma=False,
    )
```

```python
import jax
import jax.numpy as jnp
from jax import lax
from jax.experimental import pallas as pl
from jax.experimental.pallas import tpu as pltpu
from jax.sharding import PartitionSpec as P

signal_speed = 0.5
courant_number = 0.3
f32 = jnp.float32
bf16 = jnp.bfloat16
MESH = pl.DeviceIdType.MESH
VMEM = pl.BlockSpec(memory_space=pltpu.VMEM)


def halves(x):
    head = x.astype(bf16)
    return head, (x - head.astype(f32)).astype(bf16)


def grid_step(k):
    return 1 + lax.rem(k + 1, 3)


def packed_rows(block):
    return jnp.concatenate([block[8 * u : 8 * u + 8] for u in range(4)], axis=1)


def neighbours():
    i, j = lax.axis_index("gx"), lax.axis_index("gy")
    return (
        {"gx": lax.rem(i + 1, 16)},
        {"gx": lax.rem(i + 15, 16)},
        {"gy": lax.rem(j + 1, 4)},
        {"gy": lax.rem(j + 3, 4)},
    )


def side_copies(face_x, face_y, land_x, land_y, send, recv):
    pairs = (
        (face_x.at[:, 7], land_x.at[0]),
        (face_x.at[:, 0], land_x.at[1]),
        (face_y.at[1], land_y.at[0]),
        (face_y.at[0], land_y.at[1]),
    )
    return [
        remote(src, dst, send.at[n], recv.at[n], where)
        for n, ((src, dst), where) in enumerate(zip(pairs, neighbours()))
    ]


def edges():
    i, j = lax.axis_index("gx"), lax.axis_index("gy")
    return i < 15, i > 0, j < 3, j > 0


def start_sides(copies):
    for copy, there in zip(copies, edges()):
        pl.when(there)(copy.start)


def wait_sides(copies):
    up_x, down_x, up_y, down_y = edges()
    for copy, sends, comes in zip(
        copies, (up_x, down_x, up_y, down_y), (down_x, up_x, down_y, up_y)
    ):
        pl.when(sends)(copy.wait_send)
        pl.when(comes)(copy.wait_recv)


def remote(src, dst, send, recv, where):
    return pltpu.make_async_remote_copy(
        src_ref=src,
        dst_ref=dst,
        send_sem=send,
        recv_sem=recv,
        device_id=where,
        device_id_type=MESH,
    )


def interpolate(n, t, lhs, ints, floats, prod, turned):
    def two(ref):
        return jnp.concatenate(
            [ref[pl.ds(n * 8 + 2 * t, 1), :], ref[pl.ds(n * 8 + 2 * t + 1, 1), :]], axis=1
        )

    base = two(ints)
    fx, fy, fz = (two(floats.at[d]) for d in range(3))
    cz = base & 127
    cy = (base >> 7) & 15
    cx = base >> 11
    iz = lax.broadcasted_iota(jnp.int32, (128, 256), 0)
    wz = jnp.where(iz == cz, 1.0 - fz, jnp.where(iz == cz + 1, fz, 0.0))
    z_head, z_rest = halves(wz)
    both = lhs[...]
    prod[...] = jnp.dot(
        both, jnp.concatenate([z_head, z_head], axis=0), preferred_element_type=f32
    ) + jnp.dot(both, jnp.concatenate([z_rest, z_rest], axis=0), preferred_element_type=f32)
    iy = lax.broadcasted_iota(jnp.int32, (16, 256), 0)
    wy = jnp.where(iy == cy, 1.0 - fy, jnp.where(iy == cy + 1, fy, 0.0))
    wx = [jnp.where(cx == x, 1.0 - fx, jnp.where(cx + 1 == x, fx, 0.0)) for x in range(8)]
    rows = []
    for v in range(8):
        total = prod[v * 128 : v * 128 + 16, :] * wx[0]
        for x in range(1, 8):
            start = v * 128 + x * 16
            total = total + prod[start : start + 16, :] * wx[x]
        rows.append(jnp.sum(total * wy, axis=0, keepdims=True))
    values = jnp.concatenate(rows, axis=0)
    turned[pl.ds(pl.multiple_of(t * 16, 16), 16), :] = jnp.concatenate(
        [values[:, 0:128], values[:, 128:256]], axis=0
    )


def spots(ints, rr):
    cell = ints[pl.ds(rr, 1), :]
    column = cell >> 7
    lane = ((column >> 6) << 7) + (((cell & 127) + ((column & 32) << 1)) & 127)
    return column & 31, lane


def section_kernel(
    state_in, vel_in, corner_in, frac_in, target_in,
    filled, u_x, u_y, v_x, v_y,
    lhs, ints, floats, prods, turned, first, second, third, fourth, put_rows, put_lanes, acc, cells,
    face_u, face_v, state_ref, vel_ref, corner_ref, frac_ref, target_ref, loads,
    y_send, y_recv, d_send, d_recv, v_send, v_recv, u_send, u_recv,
):
    g, i, j = lax.axis_index("grp"), lax.axis_index("gx"), lax.axis_index("gy")
    state_load, corner_load, frac_load, vel_load, target_load = (
        pltpu.make_async_copy(src, dst, loads.at[n])
        for n, (src, dst) in enumerate(
            (
                (state_in, state_ref),
                (corner_in, corner_ref),
                (frac_in, frac_ref),
                (vel_in, vel_ref),
                (target_in, target_ref),
            )
        )
    )
    for load in (corner_load, frac_load, state_load, vel_load, target_load):
        load.start()
    barrier = pltpu.get_barrier_semaphore()

    @pl.loop(0, 48)
    def _(n):
        where = {"grp": lax.rem(g + 1 + n // 16, 4), "gx": lax.rem(n, 16)}
        pl.semaphore_signal(barrier, inc=1, device_id=where, device_id_type=MESH)

    for d in range(1, 4):
        where = {"gy": lax.rem(j + d, 4)}
        pl.semaphore_signal(barrier, inc=1, device_id=where, device_id_type=MESH)
    for where in neighbours()[:2]:
        pl.semaphore_signal(barrier, inc=1, device_id=where, device_id_type=MESH)

    corner_load.wait()
    frac_load.wait()
    for k in range(3):
        h = lax.rem(g + grid_step(k), 4)
        for c in range(2):
            at = slice((3 * c + k) * 8, (3 * c + k) * 8 + 8)
            here = slice(32 * c, 32 * c + 32)
            ints[at, :] = packed_rows(corner_ref[h, :, here])
            for d in range(3):
                floats[d, at, :] = packed_rows(frac_ref[d, h, :, here])

    state_load.wait()
    head, rest = halves(state_ref[...].reshape(1024, 128))
    lhs[:, 0:128] = head
    lhs[:, 128:256] = rest
    vel_load.wait()
    face_v[0] = vel_ref[:, :, 0, :]
    face_v[1] = vel_ref[:, :, 15, :]
    v_sides = side_copies(vel_ref, face_v, v_x, v_y, v_send, v_recv)

    def onward(n):
        remote(first.at[n, 0:3], second.at[n, 0:3], y_send, y_recv.at[n], {"gx": i}).wait_recv()
        for came in range(4):
            for u in range(2):
                third[pl.ds(n * 64 + u * 4 + came, 8, stride=8), :] = second[
                    n, came, u * 8 : u * 8 + 8
                ]
        c, k = n // 3, lax.rem(n, 3)

        @pl.loop(0, 8)
        def _(to):
            where = {"grp": lax.rem(g + grid_step(k), 4), "gx": c * 8 + to}
            remote(
                third.at[pl.ds(pl.multiple_of(n * 64 + to * 8, 8), 8)],
                fourth.at[pl.ds(pl.multiple_of(k * 128 + i * 8, 8), 8)],
                d_send,
                d_recv.at[k],
                where,
            ).start()

    early = (15 - i) // 8
    wait_at = 5 * early

    @pl.loop(0, 6)
    def _(n):
        @pl.loop(0, 4 // len(prods))
        def _(step):
            for m, prod in enumerate(prods):
                interpolate(n, step * len(prods) + m, lhs, ints, floats, prod, turned)

        both = jnp.concatenate([turned[0:64, 0:64], turned[0:64, 64:128]], axis=0)
        turned[0:64, :] = both.T
        for to in range(4):
            first[n, to] = turned[pl.ds(to, 16, stride=4), :]
        second[n, j] = first[n, j]

        @pl.when(n == wait_at)
        def _():
            pl.semaphore_wait(barrier, 53)
            start_sides(v_sides)

        @pl.when(n >= wait_at)
        def _():
            @pl.loop(lax.rem(n, 5) * (1 - early) + 5 * (n // 5) * (1 - early), n + 1)
            def _(m):
                for d in range(1, 4):
                    to = lax.rem(j + d, 4)
                    remote(
                        first.at[m, to], second.at[m, j], y_send, y_recv.at[m], {"gy": to}
                    ).start()

        @pl.when(n >= wait_at + 2)
        def _():
            onward(n - 2)

    target_load.wait()

    @pl.loop(0, 3)
    def _(k):
        cells[k] = packed_rows(target_ref[lax.rem(g + 4 - grid_step(k), 4)])

    @pl.loop(4 * (1 - early), 6)
    def _(n):
        onward(n)

    @pl.loop(0, 24)
    def _(n):
        k, rr = n // 8, lax.rem(n, 8)
        _, lane = spots(cells.at[k], rr)
        il = lax.broadcasted_iota(jnp.int32, (256, 256), 0)
        put_lanes[:, pl.ds(pl.multiple_of(n * 256, 256), 256)] = jnp.where(
            il == lane, 1.0, 0.0
        ).astype(bf16)

    acc[...] = jnp.zeros_like(acc)

    @pl.loop(0, 3)
    def _(k):
        mine = pl.ds(pl.multiple_of(k * 128, 128), 128)
        remote(third.at[mine], fourth.at[mine], d_send, d_recv.at[k], {"gx": i}).wait_recv()
        for u in range(2):
            for came in range(4):
                turned[pl.ds(u * 64 + came, 16, stride=4), :] = fourth[
                    pl.ds(k * 128 + u * 4 + came, 16, stride=8), :
                ]
        turned[...] = turned[...].T
        for part, put in enumerate(put_rows):
            for m in range(8 // len(put_rows)):
                r = part * (8 // len(put_rows)) + m
                row, _ = spots(cells.at[k], r)
                values = jnp.concatenate(
                    [turned[r * 8 : r * 8 + 8, :], turned[64 + r * 8 : 72 + r * 8, :]], axis=1
                )
                head = values.astype(bf16).astype(f32)
                rest = values - head
                hit = lax.broadcasted_iota(jnp.int32, (32, 256), 0) == row
                at = slice(m * 256, m * 256 + 256)
                for v in range(8):
                    put[v * 32 : v * 32 + 32, at] = jnp.where(hit, head[v : v + 1, :], 0.0).astype(
                        bf16
                    )
                    put[256 + v * 32 : 288 + v * 32, at] = jnp.where(
                        hit, rest[v : v + 1, :], 0.0
                    ).astype(bf16)
                put[512:544, at] = jnp.where(hit, 1.0, 0.0).astype(bf16)
            span = 2048 // len(put_rows)
            acc[...] += lax.dot_general(
                put[...],
                put_lanes[:, pl.ds(pl.multiple_of(k * 2048 + part * span, span), span)],
                (((1,), (1,)), ((), ())),
                preferred_element_type=f32,
            )

    spot = lax.broadcasted_iota(jnp.int32, (32, 128), 1)
    rim = (spot < 32) | (spot >= 96)
    for pair in range(2):
        span = slice(pair * 128, pair * 128 + 128)
        count = acc[512:544, span]
        for b in range(2):
            seen = pltpu.roll(count, 64, 1) if b else count
            hit = rim & (seen > 0.5)
            x = 4 * pair + 2 * b
            for v in range(8):
                new = acc[v * 32 : v * 32 + 32, span] + acc[256 + v * 32 : 288 + v * 32, span]
                if b:
                    new = pltpu.roll(new, 64, 1)
                old = state_ref[v, x : x + 2].reshape(32, 128)
                filled[v, x : x + 2] = jnp.where(hit, new, old).reshape(2, 16, 128)
    face_u[0] = filled[:, :, 0, :]
    face_u[1] = filled[:, :, 15, :]
    u_sides = side_copies(filled, face_u, u_x, u_y, u_send, u_recv)
    start_sides(u_sides)
    wait_sides(v_sides)
    wait_sides(u_sides)
    remote(first.at[:, 0:3], second.at[:, 0:3], y_send, y_recv.at[0], {"gx": i}).wait_send()
    remote(third, fourth, d_send, d_recv.at[0], {"gx": i}).wait_send()


UNROLL = 4
PARTS = 2


def section(state, velocity, corner, frac, target):
    dma = pltpu.SemaphoreType.DMA
    chunk = pltpu.VMEM((6, 4, 16, 128), f32)
    whole = pltpu.VMEM((384, 128), f32)
    return pl.pallas_call(
        section_kernel,
        out_shape=(
            jax.ShapeDtypeStruct((8, 8, 16, 128), f32),
            jax.ShapeDtypeStruct((2, 8, 16, 128), f32),
            jax.ShapeDtypeStruct((2, 8, 8, 128), f32),
            jax.ShapeDtypeStruct((2, 3, 16, 128), f32),
            jax.ShapeDtypeStruct((2, 3, 8, 128), f32),
        ),
        in_specs=[pl.BlockSpec(memory_space=pltpu.HBM)] * 5,
        out_specs=(VMEM,) * 5,
        scratch_shapes=[
            pltpu.VMEM((1024, 256), bf16),
            pltpu.VMEM((48, 128), jnp.int32),
            pltpu.VMEM((3, 48, 128), f32),
            [pltpu.VMEM((1024, 256), f32) for _ in range(UNROLL)],
            pltpu.VMEM((128, 128), f32),
            chunk,
            chunk,
            whole,
            whole,
            [pltpu.VMEM((544, 2048 // PARTS), bf16) for _ in range(PARTS)],
            pltpu.VMEM((256, 6144), bf16),
            pltpu.VMEM((544, 256), f32),
            pltpu.VMEM((3, 8, 256), jnp.int32),
            pltpu.VMEM((2, 8, 8, 128), f32),
            pltpu.VMEM((2, 3, 8, 128), f32),
            pltpu.VMEM((8, 8, 16, 128), f32),
            pltpu.VMEM((3, 8, 16, 128), f32),
            pltpu.VMEM((4, 32, 64), jnp.int32),
            pltpu.VMEM((3, 4, 32, 64), f32),
            pltpu.VMEM((4, 32, 64), jnp.int32),
            dma((5,)),
            dma,
            dma((6,)),
            dma,
            dma((3,)),
            dma((4,)),
            dma((4,)),
            dma((4,)),
            dma((4,)),
        ],
        compiler_params=pltpu.CompilerParams(
            collective_id=0, has_side_effects=True, vmem_limit_bytes=24 << 20
        ),
        name="section",
    )(state, velocity, corner, frac, target)


def face_weights(low, high):
    wave_low = jnp.minimum(jnp.minimum(low, high) - signal_speed, 0.0)
    wave_high = jnp.maximum(jnp.maximum(low, high) + signal_speed, 0.0)
    scale = courant_number / (wave_high - wave_low)
    return (
        wave_high * (low - wave_low) * scale,
        wave_low * (wave_high - high) * scale,
    )


def step_kernel(u_ref, vel_ref, ux_ref, uy_ref, vx_ref, vy_ref, out_ref):
    i, j = lax.axis_index("gx"), lax.axis_index("gy")
    lane = lax.broadcasted_iota(jnp.int32, (16, 128), 1)
    line = lax.broadcasted_iota(jnp.int32, (16, 128), 0)
    keep_low_x, keep_high_x = i > 0, i < 15
    keep_low_y, keep_high_y = j > 0, j < 3

    def plane(ref, side, v, x):
        if x < 0:
            return jnp.where(keep_low_x, side[0, v], 0.0)
        if x > 7:
            return jnp.where(keep_high_x, side[1, v], 0.0)
        return ref[v, x]

    def row(side, which, v, x):
        keep = keep_high_y if which else keep_low_y
        return jnp.where(keep, side[which, v, x : x + 1, :], 0.0)

    def prev_z(a):
        return jnp.where(lane == 0, 0.0, pltpu.roll(a, 1, 1))

    def next_z(a):
        return jnp.where(lane == 127, 0.0, pltpu.roll(a, 127, 1))

    def prev_y(a, low):
        return jnp.where(line == 0, low, pltpu.roll(a, 1, 0))

    def next_y(a, high):
        return jnp.where(line == 15, high, pltpu.roll(a, 15, 0))

    def elec(b, v):
        return (v[2] * b[1] - v[1] * b[2], v[0] * b[2] - v[2] * b[0], v[1] * b[0] - v[0] * b[1])

    speed = [[plane(vel_ref, vx_ref, d, x) for d in range(3)] for x in range(-1, 9)]
    weights_x = [face_weights(speed[x][0], speed[x + 1][0]) for x in range(9)]
    fields = [
        elec([plane(u_ref, ux_ref, 5 + d, x) for d in range(3)], speed[x + 1]) for x in range(-1, 9)
    ]
    flux_low = [
        weights_x[0][0] * plane(u_ref, ux_ref, v, -1) + weights_x[0][1] * u_ref[v, 0]
        for v in range(5)
    ]
    for x in range(8):
        here = speed[x + 1]
        low_v = [row(vy_ref, 0, d, x) for d in range(3)]
        high_v = [row(vy_ref, 1, d, x) for d in range(3)]
        y_low = face_weights(prev_y(here[1], low_v[1]), here[1])
        y_high = face_weights(here[1], next_y(here[1], high_v[1]))
        z_low = face_weights(prev_z(here[2]), here[2])
        z_high = face_weights(here[2], next_z(here[2]))
        centre = (
            1.0
            + y_low[1] - y_high[0]
            + z_low[1] - z_high[0]
        )
        for v in range(5):
            u = u_ref[v, x]
            flux_high = weights_x[x + 1][0] * u + weights_x[x + 1][1] * plane(
                u_ref, ux_ref, v, x + 1
            )
            new = centre * u - (flux_high - flux_low[v])
            flux_low[v] = flux_high
            new = new + y_low[0] * prev_y(u, row(uy_ref, 0, v, x))
            new = new - y_high[1] * next_y(u, row(uy_ref, 1, v, x))
            new = new + z_low[0] * prev_z(u)
            new = new - z_high[1] * next_z(u)
            out_ref[v, x] = new
        below, e, above = fields[x], fields[x + 1], fields[x + 2]
        e_low = elec([row(uy_ref, 0, 5 + d, x) for d in range(3)], low_v)
        e_high = elec([row(uy_ref, 1, 5 + d, x) for d in range(3)], high_v)

        def along_y(d):
            return next_y(e[d], e_high[d]) - prev_y(e[d], e_low[d])

        def along_z(d):
            return next_z(e[d]) - prev_z(e[d])

        def along_x(d):
            return above[d] - below[d]

        half = 0.5 * courant_number
        out_ref[5, x] = u_ref[5, x] - half * (along_y(2) - along_z(1))
        out_ref[6, x] = u_ref[6, x] - half * (along_z(0) - along_x(2))
        out_ref[7, x] = u_ref[7, x] - half * (along_x(1) - along_y(0))


def step(u, vel, ux, uy, vx, vy):
    return pl.pallas_call(
        step_kernel,
        out_shape=jax.ShapeDtypeStruct((8, 8, 16, 128), f32),
        in_specs=[VMEM] * 6,
        out_specs=VMEM,
        compiler_params=pltpu.CompilerParams(vmem_limit_bytes=8 << 20),
        name="step",
    )(u, vel, ux, uy, vx, vy)


def per_device(conserved, velocity, donor_corner, donor_fraction, target_cell):
    state = conserved[:, 0]
    speeds = velocity[:, 0]
    corner = donor_corner[0, 0, 0].transpose(0, 2, 1)
    frac = donor_fraction[:, 0, 0, 0].transpose(0, 1, 3, 2)
    target = target_cell[0, 0, 0].transpose(0, 2, 1)
    state, far_speeds, corner, frac, target = (
        pltpu.with_memory_space_constraint(x, pltpu.HBM) for x in (state, speeds, corner, frac, target)
    )
    filled, u_x, u_y, v_x, v_y = section(state, far_speeds, corner, frac, target)
    return step(filled, speeds, u_x, u_y, v_x, v_y)[:, None]


def solution(mesh):
    return jax.shard_map(
        per_device,
        mesh=mesh,
        in_specs=(
            P(None, "grp", "gx", "gy", None),
            P(None, "grp", "gx", "gy", None),
            P("grp", "gx", "gy", None, None, None),
            P(None, "grp", "gx", "gy", None, None, None),
            P("grp", "gx", "gy", None, None, None),
        ),
        out_specs=P(None, "grp", "gx", "gy", None),
        check_vma=False,
    )
```

```python
import jax
import jax.numpy as jnp
from jax import lax
from jax.experimental import pallas as pl
from jax.experimental.pallas import tpu as pltpu
from jax.sharding import PartitionSpec as P

signal_speed = 0.5
courant_number = 0.3
f32 = jnp.float32
bf16 = jnp.bfloat16
MESH = pl.DeviceIdType.MESH
VMEM = pl.BlockSpec(memory_space=pltpu.VMEM)


def halves(x):
    head = x.astype(bf16)
    return head, (x - head.astype(f32)).astype(bf16)


def grid_step(k):
    return 1 + lax.rem(k + 1, 3)


def meetings(g):
    return 3 - g // 2


def send_slot(g, m):
    return m * (1 + g // 3)


def take_slot(g, m):
    return m * (1 + (g // 2) * (3 - g))


def packed_rows(block):
    return jnp.concatenate([block[8 * u : 8 * u + 8] for u in range(4)], axis=1)


def neighbours():
    i, j = lax.axis_index("gx"), lax.axis_index("gy")
    return (
        {"gx": lax.rem(i + 1, 16)},
        {"gx": lax.rem(i + 15, 16)},
        {"gy": lax.rem(j + 1, 4)},
        {"gy": lax.rem(j + 3, 4)},
    )


def side_copies(face_x, face_y, land_x, land_y, send, recv):
    pairs = (
        (face_x.at[:, 7], land_x.at[0]),
        (face_x.at[:, 0], land_x.at[1]),
        (face_y.at[1], land_y.at[0]),
        (face_y.at[0], land_y.at[1]),
    )
    return [
        remote(src, dst, send.at[n], recv.at[n], where)
        for n, ((src, dst), where) in enumerate(zip(pairs, neighbours()))
    ]


def edges():
    i, j = lax.axis_index("gx"), lax.axis_index("gy")
    return i < 15, i > 0, j < 3, j > 0


def start_sides(copies):
    for copy, there in zip(copies, edges()):
        pl.when(there)(copy.start)


def wait_sides(copies):
    up_x, down_x, up_y, down_y = edges()
    for copy, sends, comes in zip(
        copies, (up_x, down_x, up_y, down_y), (down_x, up_x, down_y, up_y)
    ):
        pl.when(sends)(copy.wait_send)
        pl.when(comes)(copy.wait_recv)


def remote(src, dst, send, recv, where):
    return pltpu.make_async_remote_copy(
        src_ref=src,
        dst_ref=dst,
        send_sem=send,
        recv_sem=recv,
        device_id=where,
        device_id_type=MESH,
    )


def interpolate(n, t, lhs, ints, floats, prod, turned):
    def two(ref):
        return jnp.concatenate(
            [ref[pl.ds(n * 8 + 2 * t, 1), :], ref[pl.ds(n * 8 + 2 * t + 1, 1), :]], axis=1
        )

    base = two(ints)
    fx, fy, fz = (two(floats.at[d]) for d in range(3))
    cz = base & 127
    cy = (base >> 7) & 15
    cx = base >> 11
    iz = lax.broadcasted_iota(jnp.int32, (128, 256), 0)
    wz = jnp.where(iz == cz, 1.0 - fz, jnp.where(iz == cz + 1, fz, 0.0))
    z_head, z_rest = halves(wz)
    both = lhs[...]
    prod[...] = jnp.dot(
        both, jnp.concatenate([z_head, z_head], axis=0), preferred_element_type=f32
    ) + jnp.dot(both, jnp.concatenate([z_rest, z_rest], axis=0), preferred_element_type=f32)
    iy = lax.broadcasted_iota(jnp.int32, (16, 256), 0)
    wy = jnp.where(iy == cy, 1.0 - fy, jnp.where(iy == cy + 1, fy, 0.0))
    wx = [jnp.where(cx == x, 1.0 - fx, jnp.where(cx + 1 == x, fx, 0.0)) for x in range(8)]
    rows = []
    for v in range(8):
        total = prod[v * 128 : v * 128 + 16, :] * wx[0]
        for x in range(1, 8):
            start = v * 128 + x * 16
            total = total + prod[start : start + 16, :] * wx[x]
        rows.append(jnp.sum(total * wy, axis=0, keepdims=True))
    values = jnp.concatenate(rows, axis=0)
    turned[pl.ds(pl.multiple_of(t * 16, 16), 16), :] = jnp.concatenate(
        [values[:, 0:128], values[:, 128:256]], axis=0
    )


def spots(ints, rr):
    cell = ints[pl.ds(rr, 1), :]
    column = cell >> 7
    lane = ((column >> 6) << 7) + (((cell & 127) + ((column & 32) << 1)) & 127)
    return column & 31, lane


def section_kernel(
    state_in, vel_in, corner_in, frac_in, target_in,
    filled, u_x, u_y, v_x, v_y,
    lhs, ints, floats, prods, turned, first, second, third, fourth, put_rows, put_lanes, acc, cells,
    face_u, face_v, state_ref, vel_ref, corner_ref, frac_ref, target_ref, loads,
    y_send, y_recv, d_send, d_recv, v_send, v_recv, u_send, u_recv,
):
    g, i, j = lax.axis_index("grp"), lax.axis_index("gx"), lax.axis_index("gy")
    state_load, corner_load, frac_load, vel_load, target_load = (
        pltpu.make_async_copy(src, dst, loads.at[n])
        for n, (src, dst) in enumerate(
            (
                (state_in, state_ref),
                (corner_in, corner_ref),
                (frac_in, frac_ref),
                (vel_in, vel_ref),
                (target_in, target_ref),
            )
        )
    )
    for load in (corner_load, frac_load, state_load, vel_load, target_load):
        load.start()
    barrier = pltpu.get_barrier_semaphore()

    met = meetings(g)

    grids = [lax.rem(g + grid_step(send_slot(g, m)), 4) for m in range(3)]

    def greet(m):
        @pl.loop(0, 16, unroll=8)
        def _(to):
            where = {"grp": grids[m], "gx": to}
            pl.semaphore_signal(barrier, inc=1, device_id=where, device_id_type=MESH)

    greet(0)
    greet(1)

    @pl.when(met == 3)
    def _():
        greet(2)

    for d in range(1, 4):
        where = {"gy": lax.rem(j + d, 4)}
        pl.semaphore_signal(barrier, inc=1, device_id=where, device_id_type=MESH)
    for where in neighbours()[:2]:
        pl.semaphore_signal(barrier, inc=1, device_id=where, device_id_type=MESH)

    corner_load.wait()
    frac_load.wait()
    @pl.loop(0, met)
    def _(m):
        h = lax.rem(g + grid_step(send_slot(g, m)), 4)
        for c in range(2):
            at = pl.ds(pl.multiple_of((c * met + m) * 8, 8), 8)
            here = slice(32 * c, 32 * c + 32)
            ints[at, :] = packed_rows(corner_ref[h, :, here])
            for d in range(3):
                floats[d, at, :] = packed_rows(frac_ref[d, h, :, here])

    state_load.wait()
    head, rest = halves(state_ref[...].reshape(1024, 128))
    lhs[:, 0:128] = head
    lhs[:, 128:256] = rest
    v_sides = side_copies(vel_ref, face_v, v_x, v_y, v_send, v_recv)

    def onward(n):
        remote(first.at[n, 0:3], second.at[n, 0:3], y_send, y_recv.at[n], {"gx": i}).wait_recv()
        for came in range(4):
            for u in range(2):
                third[pl.ds(n * 64 + u * 4 + came, 8, stride=8), :] = second[
                    n, came, u * 8 : u * 8 + 8
                ]
        c = n // met
        k = send_slot(g, n - c * met)

        grid = lax.rem(g + grid_step(k), 4)

        @pl.loop(0, 8, unroll=8)
        def _(to):
            where = {"grp": grid, "gx": c * 8 + to}
            remote(
                third.at[pl.ds(pl.multiple_of(n * 64 + to * 8, 8), 8)],
                fourth.at[pl.ds(pl.multiple_of(k * 128 + i * 8, 8), 8)],
                d_send,
                d_recv.at[k],
                where,
            ).start()

    early = (15 - i) // 8
    chunks = 2 * met
    wait_at = (chunks - 1) * early

    @pl.loop(0, chunks)
    def _(n):
        @pl.loop(0, 4 // len(prods))
        def _(step):
            for m, prod in enumerate(prods):
                interpolate(n, step * len(prods) + m, lhs, ints, floats, prod, turned)

        both = jnp.concatenate([turned[0:64, 0:64], turned[0:64, 64:128]], axis=0)
        turned[0:64, :] = both.T
        for to in range(4):
            first[n, to] = turned[pl.ds(to, 16, stride=4), :]
        second[n, j] = first[n, j]

        @pl.when(n == wait_at)
        def _():
            pl.semaphore_wait(barrier, 16 * met + 5)

        @pl.when(n >= wait_at)
        def _():
            @pl.loop(lax.rem(n, 5) * (1 - early) + 5 * (n // 5) * (1 - early), n + 1)
            def _(m):
                for d in range(1, 4):
                    to = lax.rem(j + d, 4)
                    remote(
                        first.at[m, to], second.at[m, j], y_send, y_recv.at[m], {"gy": to}
                    ).start()

        @pl.when(n >= wait_at + 2)
        def _():
            onward(n - 2)

    target_load.wait()

    @pl.loop(0, met)
    def _(m):
        cells[m] = packed_rows(target_ref[lax.rem(g + 4 - grid_step(take_slot(g, m)), 4)])

    @pl.loop((chunks - 2) * (1 - early), chunks)
    def _(n):
        onward(n)

    vel_load.wait()
    face_v[0] = vel_ref[:, :, 0, :]
    face_v[1] = vel_ref[:, :, 15, :]
    start_sides(v_sides)

    @pl.loop(0, 8 * met)
    def _(n):
        k, rr = n // 8, lax.rem(n, 8)
        _, lane = spots(cells.at[k], rr)
        il = lax.broadcasted_iota(jnp.int32, (256, 256), 0)
        put_lanes[:, pl.ds(pl.multiple_of(n * 256, 256), 256)] = jnp.where(
            il == lane, 1.0, 0.0
        ).astype(bf16)

    acc[...] = jnp.zeros_like(acc)

    @pl.loop(0, met)
    def _(n):
        k = take_slot(g, n)
        mine = pl.ds(pl.multiple_of(k * 128, 128), 128)
        remote(third.at[mine], fourth.at[mine], d_send, d_recv.at[k], {"gx": i}).wait_recv()
        for u in range(2):
            for came in range(4):
                turned[pl.ds(u * 64 + came, 16, stride=4), :] = fourth[
                    pl.ds(k * 128 + u * 4 + came, 16, stride=8), :
                ]
        turned[...] = turned[...].T
        for part, put in enumerate(put_rows):
            for m in range(8 // len(put_rows)):
                r = part * (8 // len(put_rows)) + m
                row, _ = spots(cells.at[n], r)
                values = jnp.concatenate(
                    [turned[r * 8 : r * 8 + 8, :], turned[64 + r * 8 : 72 + r * 8, :]], axis=1
                )
                head = values.astype(bf16).astype(f32)
                rest = values - head
                hit = lax.broadcasted_iota(jnp.int32, (32, 256), 0) == row
                at = slice(m * 256, m * 256 + 256)
                for v in range(8):
                    put[v * 32 : v * 32 + 32, at] = jnp.where(hit, head[v : v + 1, :], 0.0).astype(
                        bf16
                    )
                    put[256 + v * 32 : 288 + v * 32, at] = jnp.where(
                        hit, rest[v : v + 1, :], 0.0
                    ).astype(bf16)
                put[512:544, at] = jnp.where(hit, 1.0, 0.0).astype(bf16)
            span = 2048 // len(put_rows)
            acc[...] += lax.dot_general(
                put[...],
                put_lanes[:, pl.ds(pl.multiple_of(n * 2048 + part * span, span), span)],
                (((1,), (1,)), ((), ())),
                preferred_element_type=f32,
            )

    spot = lax.broadcasted_iota(jnp.int32, (32, 128), 1)
    rim = (spot < 32) | (spot >= 96)
    for pair in range(2):
        span = slice(pair * 128, pair * 128 + 128)
        count = acc[512:544, span]
        for b in range(2):
            seen = pltpu.roll(count, 64, 1) if b else count
            hit = rim & (seen > 0.5)
            x = 4 * pair + 2 * b
            for v in range(8):
                new = acc[v * 32 : v * 32 + 32, span] + acc[256 + v * 32 : 288 + v * 32, span]
                if b:
                    new = pltpu.roll(new, 64, 1)
                old = state_ref[v, x : x + 2].reshape(32, 128)
                filled[v, x : x + 2] = jnp.where(hit, new, old).reshape(2, 16, 128)
    face_u[0] = filled[:, :, 0, :]
    face_u[1] = filled[:, :, 15, :]
    u_sides = side_copies(filled, face_u, u_x, u_y, u_send, u_recv)
    start_sides(u_sides)
    wait_sides(v_sides)
    wait_sides(u_sides)

    @pl.loop(0, chunks)
    def _(n):
        remote(first.at[n, 0:3], second.at[n, 0:3], y_send, y_recv.at[n], {"gx": i}).wait_send()
        mine = pl.ds(pl.multiple_of(n * 64, 64), 64)
        remote(third.at[mine], fourth.at[mine], d_send, d_recv.at[0], {"gx": i}).wait_send()


UNROLL = 4
PARTS = 2


def section(state, velocity, corner, frac, target):
    dma = pltpu.SemaphoreType.DMA
    chunk = pltpu.VMEM((6, 4, 16, 128), f32)
    whole = pltpu.VMEM((384, 128), f32)
    return pl.pallas_call(
        section_kernel,
        out_shape=(
            jax.ShapeDtypeStruct((8, 8, 16, 128), f32),
            jax.ShapeDtypeStruct((2, 8, 16, 128), f32),
            jax.ShapeDtypeStruct((2, 8, 8, 128), f32),
            jax.ShapeDtypeStruct((2, 3, 16, 128), f32),
            jax.ShapeDtypeStruct((2, 3, 8, 128), f32),
        ),
        in_specs=[pl.BlockSpec(memory_space=pltpu.HBM)] * 5,
        out_specs=(VMEM,) * 5,
        scratch_shapes=[
            pltpu.VMEM((1024, 256), bf16),
            pltpu.VMEM((48, 128), jnp.int32),
            pltpu.VMEM((3, 48, 128), f32),
            [pltpu.VMEM((1024, 256), f32) for _ in range(UNROLL)],
            pltpu.VMEM((128, 128), f32),
            chunk,
            chunk,
            whole,
            whole,
            [pltpu.VMEM((544, 2048 // PARTS), bf16) for _ in range(PARTS)],
            pltpu.VMEM((256, 6144), bf16),
            pltpu.VMEM((544, 256), f32),
            pltpu.VMEM((3, 8, 256), jnp.int32),
            pltpu.VMEM((2, 8, 8, 128), f32),
            pltpu.VMEM((2, 3, 8, 128), f32),
            pltpu.VMEM((8, 8, 16, 128), f32),
            pltpu.VMEM((3, 8, 16, 128), f32),
            pltpu.VMEM((4, 32, 64), jnp.int32),
            pltpu.VMEM((3, 4, 32, 64), f32),
            pltpu.VMEM((4, 32, 64), jnp.int32),
            dma((5,)),
            dma,
            dma((6,)),
            dma,
            dma((3,)),
            dma((4,)),
            dma((4,)),
            dma((4,)),
            dma((4,)),
        ],
        compiler_params=pltpu.CompilerParams(
            collective_id=0, has_side_effects=True, vmem_limit_bytes=24 << 20
        ),
        name="section",
    )(state, velocity, corner, frac, target)


def face_weights(low, high):
    wave_low = jnp.minimum(jnp.minimum(low, high) - signal_speed, 0.0)
    wave_high = jnp.maximum(jnp.maximum(low, high) + signal_speed, 0.0)
    scale = courant_number / (wave_high - wave_low)
    return (
        wave_high * (low - wave_low) * scale,
        wave_low * (wave_high - high) * scale,
    )


def step_kernel(u_ref, vel_ref, ux_ref, uy_ref, vx_ref, vy_ref, out_ref):
    i, j = lax.axis_index("gx"), lax.axis_index("gy")
    lane = lax.broadcasted_iota(jnp.int32, (16, 128), 1)
    line = lax.broadcasted_iota(jnp.int32, (16, 128), 0)
    keep_low_x, keep_high_x = i > 0, i < 15
    keep_low_y, keep_high_y = j > 0, j < 3

    def plane(ref, side, v, x):
        if x < 0:
            return jnp.where(keep_low_x, side[0, v], 0.0)
        if x > 7:
            return jnp.where(keep_high_x, side[1, v], 0.0)
        return ref[v, x]

    def row(side, which, v, x):
        keep = keep_high_y if which else keep_low_y
        return jnp.where(keep, side[which, v, x : x + 1, :], 0.0)

    def prev_z(a):
        return jnp.where(lane == 0, 0.0, pltpu.roll(a, 1, 1))

    def next_z(a):
        return jnp.where(lane == 127, 0.0, pltpu.roll(a, 127, 1))

    def prev_y(a, low):
        return jnp.where(line == 0, low, pltpu.roll(a, 1, 0))

    def next_y(a, high):
        return jnp.where(line == 15, high, pltpu.roll(a, 15, 0))

    def elec(b, v):
        return (v[2] * b[1] - v[1] * b[2], v[0] * b[2] - v[2] * b[0], v[1] * b[0] - v[0] * b[1])

    speed = [[plane(vel_ref, vx_ref, d, x) for d in range(3)] for x in range(-1, 9)]
    weights_x = [face_weights(speed[x][0], speed[x + 1][0]) for x in range(9)]
    fields = [
        elec([plane(u_ref, ux_ref, 5 + d, x) for d in range(3)], speed[x + 1]) for x in range(-1, 9)
    ]
    flux_low = [
        weights_x[0][0] * plane(u_ref, ux_ref, v, -1) + weights_x[0][1] * u_ref[v, 0]
        for v in range(5)
    ]
    for x in range(8):
        here = speed[x + 1]
        low_v = [row(vy_ref, 0, d, x) for d in range(3)]
        high_v = [row(vy_ref, 1, d, x) for d in range(3)]
        y_low = face_weights(prev_y(here[1], low_v[1]), here[1])
        y_high = face_weights(here[1], next_y(here[1], high_v[1]))
        z_low = face_weights(prev_z(here[2]), here[2])
        z_high = face_weights(here[2], next_z(here[2]))
        centre = (
            1.0
            + y_low[1] - y_high[0]
            + z_low[1] - z_high[0]
        )
        for v in range(5):
            u = u_ref[v, x]
            flux_high = weights_x[x + 1][0] * u + weights_x[x + 1][1] * plane(
                u_ref, ux_ref, v, x + 1
            )
            new = centre * u - (flux_high - flux_low[v])
            flux_low[v] = flux_high
            new = new + y_low[0] * prev_y(u, row(uy_ref, 0, v, x))
            new = new - y_high[1] * next_y(u, row(uy_ref, 1, v, x))
            new = new + z_low[0] * prev_z(u)
            new = new - z_high[1] * next_z(u)
            out_ref[v, x] = new
        below, e, above = fields[x], fields[x + 1], fields[x + 2]
        e_low = elec([row(uy_ref, 0, 5 + d, x) for d in range(3)], low_v)
        e_high = elec([row(uy_ref, 1, 5 + d, x) for d in range(3)], high_v)

        def along_y(d):
            return next_y(e[d], e_high[d]) - prev_y(e[d], e_low[d])

        def along_z(d):
            return next_z(e[d]) - prev_z(e[d])

        def along_x(d):
            return above[d] - below[d]

        half = 0.5 * courant_number
        out_ref[5, x] = u_ref[5, x] - half * (along_y(2) - along_z(1))
        out_ref[6, x] = u_ref[6, x] - half * (along_z(0) - along_x(2))
        out_ref[7, x] = u_ref[7, x] - half * (along_x(1) - along_y(0))


def step(u, vel, ux, uy, vx, vy):
    return pl.pallas_call(
        step_kernel,
        out_shape=jax.ShapeDtypeStruct((8, 8, 16, 128), f32),
        in_specs=[VMEM] * 6,
        out_specs=VMEM,
        compiler_params=pltpu.CompilerParams(vmem_limit_bytes=8 << 20),
        name="step",
    )(u, vel, ux, uy, vx, vy)


def per_device(conserved, velocity, donor_corner, donor_fraction, target_cell):
    state = conserved[:, 0]
    speeds = velocity[:, 0]
    corner = donor_corner[0, 0, 0].transpose(0, 2, 1)
    frac = donor_fraction[:, 0, 0, 0].transpose(0, 1, 3, 2)
    target = target_cell[0, 0, 0].transpose(0, 2, 1)
    state, far_speeds, corner, frac, target = (
        pltpu.with_memory_space_constraint(x, pltpu.HBM) for x in (state, speeds, corner, frac, target)
    )
    filled, u_x, u_y, v_x, v_y = section(state, far_speeds, corner, frac, target)
    return step(filled, speeds, u_x, u_y, v_x, v_y)[:, None]


def solution(mesh):
    return jax.shard_map(
        per_device,
        mesh=mesh,
        in_specs=(
            P(None, "grp", "gx", "gy", None),
            P(None, "grp", "gx", "gy", None),
            P("grp", "gx", "gy", None, None, None),
            P(None, "grp", "gx", "gy", None, None, None),
            P("grp", "gx", "gy", None, None, None),
        ),
        out_specs=P(None, "grp", "gx", "gy", None),
        check_vma=False,
    )
```

```python
import jax
import jax.numpy as jnp
from jax import lax
from jax.experimental import pallas as pl
from jax.experimental.pallas import tpu as pltpu
from jax.sharding import PartitionSpec as P

signal_speed = 0.5
courant_number = 0.3
f32 = jnp.float32
bf16 = jnp.bfloat16
MESH = pl.DeviceIdType.MESH
VMEM = pl.BlockSpec(memory_space=pltpu.VMEM)


def halves(x):
    head = x.astype(bf16)
    return head, (x - head.astype(f32)).astype(bf16)


def grid_step(k):
    return 1 + lax.rem(k + 1, 3)


def meetings(g):
    return 3 - g // 2


def send_slot(g, m):
    return m * (1 + g // 3)


def take_slot(g, m):
    return m * (1 + (g // 2) * (3 - g))


def packed_rows(block):
    return jnp.concatenate([block[8 * u : 8 * u + 8] for u in range(4)], axis=1)


def neighbours():
    i, j = lax.axis_index("gx"), lax.axis_index("gy")
    return (
        {"gx": lax.rem(i + 1, 16)},
        {"gx": lax.rem(i + 15, 16)},
        {"gy": lax.rem(j + 1, 4)},
        {"gy": lax.rem(j + 3, 4)},
    )


def side_copies(face_x, face_y, land_x, land_y, send, recv):
    pairs = (
        (face_x.at[:, 7], land_x.at[0]),
        (face_x.at[:, 0], land_x.at[1]),
        (face_y.at[1], land_y.at[0]),
        (face_y.at[0], land_y.at[1]),
    )
    return [
        remote(src, dst, send.at[n], recv.at[n], where)
        for n, ((src, dst), where) in enumerate(zip(pairs, neighbours()))
    ]


def edges():
    i, j = lax.axis_index("gx"), lax.axis_index("gy")
    return i < 15, i > 0, j < 3, j > 0


def start_sides(copies):
    for copy, there in zip(copies, edges()):
        pl.when(there)(copy.start)


def wait_sides(copies):
    up_x, down_x, up_y, down_y = edges()
    for copy, sends, comes in zip(
        copies, (up_x, down_x, up_y, down_y), (down_x, up_x, down_y, up_y)
    ):
        pl.when(sends)(copy.wait_send)
        pl.when(comes)(copy.wait_recv)


def remote(src, dst, send, recv, where):
    return pltpu.make_async_remote_copy(
        src_ref=src,
        dst_ref=dst,
        send_sem=send,
        recv_sem=recv,
        device_id=where,
        device_id_type=MESH,
    )


def interpolate(n, t, lhs, ints, floats, prod, turned):
    def two(ref):
        return jnp.concatenate(
            [ref[pl.ds(n * 8 + 2 * t, 1), :], ref[pl.ds(n * 8 + 2 * t + 1, 1), :]], axis=1
        )

    base = two(ints)
    fx, fy, fz = (two(floats.at[d]) for d in range(3))
    cz = base & 127
    cy = (base >> 7) & 15
    cx = base >> 11
    iz = lax.broadcasted_iota(jnp.int32, (128, 256), 0)
    wz = jnp.where(iz == cz, 1.0 - fz, jnp.where(iz == cz + 1, fz, 0.0))
    z_head, z_rest = halves(wz)
    both = lhs[...]
    prod[...] = jnp.dot(
        both, jnp.concatenate([z_head, z_head], axis=0), preferred_element_type=f32
    ) + jnp.dot(both, jnp.concatenate([z_rest, z_rest], axis=0), preferred_element_type=f32)
    iy = lax.broadcasted_iota(jnp.int32, (16, 256), 0)
    wy = jnp.where(iy == cy, 1.0 - fy, jnp.where(iy == cy + 1, fy, 0.0))
    wx = [jnp.where(cx == x, 1.0 - fx, jnp.where(cx + 1 == x, fx, 0.0)) for x in range(8)]
    rows = []
    for v in range(8):
        total = prod[v * 128 : v * 128 + 16, :] * wx[0]
        for x in range(1, 8):
            start = v * 128 + x * 16
            total = total + prod[start : start + 16, :] * wx[x]
        rows.append(jnp.sum(total * wy, axis=0, keepdims=True))
    values = jnp.concatenate(rows, axis=0)
    turned[pl.ds(pl.multiple_of(t * 16, 16), 16), :] = jnp.concatenate(
        [values[:, 0:128], values[:, 128:256]], axis=0
    )


def spots(ints, rr):
    cell = ints[pl.ds(rr, 1), :]
    column = cell >> 7
    lane = ((column >> 6) << 7) + (((cell & 127) + ((column & 32) << 1)) & 127)
    return column & 31, lane


def section_kernel(
    state_in, vel_in, corner_in, frac_in, target_in,
    filled, u_x, u_y, v_x, v_y,
    lhs, ints, floats, prods, turned, first, second, third, fourth, put_rows, put_lanes, acc, cells,
    face_u, face_v, state_ref, vel_ref, corner_ref, frac_ref, target_ref, loads,
    ready, y_send, y_recv, d_send, d_recv, v_send, v_recv, u_send, u_recv,
):
    g, i, j = lax.axis_index("grp"), lax.axis_index("gx"), lax.axis_index("gy")
    state_load, corner_load, frac_load, vel_load, target_load = (
        pltpu.make_async_copy(src, dst, loads.at[n])
        for n, (src, dst) in enumerate(
            (
                (state_in, state_ref),
                (corner_in, corner_ref),
                (frac_in, frac_ref),
                (vel_in, vel_ref),
                (target_in, target_ref),
            )
        )
    )
    for load in (corner_load, frac_load, state_load, vel_load, target_load):
        load.start()
    barrier = pltpu.get_barrier_semaphore()

    met = meetings(g)

    early = (15 - i) // 8
    grids = [lax.rem(g + grid_step(send_slot(g, m)), 4) for m in range(3)]

    def greet(m, semaphore, first_to):
        @pl.loop(0, 8, unroll=8)
        def _(to):
            where = {"grp": grids[m], "gx": first_to + to}
            pl.semaphore_signal(semaphore, inc=1, device_id=where, device_id_type=MESH)

    def greet_half(semaphore, first_to):
        greet(0, semaphore, first_to)
        greet(1, semaphore, first_to)

        @pl.when(met == 3)
        def _():
            greet(2, semaphore, first_to)

    @pl.when(early == 1)
    def _():
        greet_half(barrier, 0)

    greet_half(barrier, 8)
    for d in range(1, 4):
        where = {"gy": lax.rem(j + d, 4)}
        pl.semaphore_signal(barrier, inc=1, device_id=where, device_id_type=MESH)

    @pl.when(i < 15)
    def _():
        pl.semaphore_signal(barrier, inc=1, device_id={"gx": i + 1}, device_id_type=MESH)

    @pl.when(i > 0)
    def _():
        pl.semaphore_signal(barrier, inc=1, device_id={"gx": i - 1}, device_id_type=MESH)

    greeted = 8 * met * (2 - early) + 5 - (15 - i) // 15 - i // 15

    corner_load.wait()
    frac_load.wait()
    @pl.loop(0, met)
    def _(m):
        h = lax.rem(g + grid_step(send_slot(g, m)), 4)
        for c in range(2):
            at = pl.ds(pl.multiple_of((c * met + m) * 8, 8), 8)
            here = slice(32 * c, 32 * c + 32)
            ints[at, :] = packed_rows(corner_ref[h, :, here])
            for d in range(3):
                floats[d, at, :] = packed_rows(frac_ref[d, h, :, here])

    state_load.wait()
    head, rest = halves(state_ref[...].reshape(1024, 128))
    lhs[:, 0:128] = head
    lhs[:, 128:256] = rest
    v_sides = side_copies(vel_ref, face_v, v_x, v_y, v_send, v_recv)

    def onward(n):
        remote(first.at[n, 0:3], second.at[n, 0:3], y_send, y_recv.at[n], {"gx": i}).wait_recv()
        for came in range(4):
            for u in range(2):
                third[pl.ds(n * 64 + u * 4 + came, 8, stride=8), :] = second[
                    n, came, u * 8 : u * 8 + 8
                ]
        c = n // met
        k = send_slot(g, n - c * met)

        grid = lax.rem(g + grid_step(k), 4)

        @pl.loop(0, 8, unroll=8)
        def _(to):
            where = {"grp": grid, "gx": c * 8 + to}
            remote(
                third.at[pl.ds(pl.multiple_of(n * 64 + to * 8, 8), 8)],
                fourth.at[pl.ds(pl.multiple_of(k * 128 + i * 8, 8), 8)],
                d_send,
                d_recv.at[k],
                where,
            ).start()

    chunks = 2 * met
    wait_at = 1 + (met - 2) * early

    @pl.loop(0, chunks)
    def _(n):
        @pl.loop(0, 4 // len(prods))
        def _(step):
            for m, prod in enumerate(prods):
                interpolate(n, step * len(prods) + m, lhs, ints, floats, prod, turned)

        both = jnp.concatenate([turned[0:64, 0:64], turned[0:64, 64:128]], axis=0)
        turned[0:64, :] = both.T
        for to in range(4):
            first[n, to] = turned[pl.ds(to, 16, stride=4), :]
        second[n, j] = first[n, j]

        @pl.when(n == wait_at)
        def _():
            pl.semaphore_wait(barrier, greeted)

            @pl.when(early == 0)
            def _():
                greet_half(ready, 0)

        def along(m):
            for d in range(1, 4):
                to = lax.rem(j + d, 4)
                remote(
                    first.at[m, to], second.at[m, j], y_send, y_recv.at[m], {"gy": to}
                ).start()

        @pl.when(n == wait_at)
        def _():
            pl.loop(0, n + 1)(along)

        @pl.when(n > wait_at)
        def _():
            along(n)

        @pl.when(n * early == met + 1)
        def _():
            pl.loop(0, met)(onward)

        @pl.when(n * (1 - early) == 3)
        def _():
            onward(0)

        @pl.when(n * (1 - early) >= 3)
        def _():
            onward(n - 2)

    target_load.wait()

    @pl.loop(0, met)
    def _(m):
        cells[m] = packed_rows(target_ref[lax.rem(g + 4 - grid_step(take_slot(g, m)), 4)])

    @pl.loop((chunks - 2) * (1 - early) + met * early, chunks)
    def _(n):
        @pl.when(n == met + chunks * (1 - early))
        def _():
            pl.semaphore_wait(ready, 8 * met)

        onward(n)

    vel_load.wait()
    face_v[0] = vel_ref[:, :, 0, :]
    face_v[1] = vel_ref[:, :, 15, :]
    start_sides(v_sides)

    @pl.loop(0, 8 * met)
    def _(n):
        k, rr = n // 8, lax.rem(n, 8)
        _, lane = spots(cells.at[k], rr)
        il = lax.broadcasted_iota(jnp.int32, (256, 256), 0)
        put_lanes[:, pl.ds(pl.multiple_of(n * 256, 256), 256)] = jnp.where(
            il == lane, 1.0, 0.0
        ).astype(bf16)

    acc[...] = jnp.zeros_like(acc)

    @pl.loop(0, met)
    def _(n):
        k = take_slot(g, n)
        mine = pl.ds(pl.multiple_of(k * 128, 128), 128)
        remote(third.at[mine], fourth.at[mine], d_send, d_recv.at[k], {"gx": i}).wait_recv()
        for u in range(2):
            for came in range(4):
                turned[pl.ds(u * 64 + came, 16, stride=4), :] = fourth[
                    pl.ds(k * 128 + u * 4 + came, 16, stride=8), :
                ]
        turned[...] = turned[...].T
        for part, put in enumerate(put_rows):
            for m in range(8 // len(put_rows)):
                r = part * (8 // len(put_rows)) + m
                row, _ = spots(cells.at[n], r)
                values = jnp.concatenate(
                    [turned[r * 8 : r * 8 + 8, :], turned[64 + r * 8 : 72 + r * 8, :]], axis=1
                )
                head = values.astype(bf16).astype(f32)
                rest = values - head
                hit = lax.broadcasted_iota(jnp.int32, (32, 256), 0) == row
                at = slice(m * 256, m * 256 + 256)
                for v in range(8):
                    put[v * 32 : v * 32 + 32, at] = jnp.where(hit, head[v : v + 1, :], 0.0).astype(
                        bf16
                    )
                    put[256 + v * 32 : 288 + v * 32, at] = jnp.where(
                        hit, rest[v : v + 1, :], 0.0
                    ).astype(bf16)
                put[512:544, at] = jnp.where(hit, 1.0, 0.0).astype(bf16)
            span = 2048 // len(put_rows)
            acc[...] += lax.dot_general(
                put[...],
                put_lanes[:, pl.ds(pl.multiple_of(n * 2048 + part * span, span), span)],
                (((1,), (1,)), ((), ())),
                preferred_element_type=f32,
            )

    spot = lax.broadcasted_iota(jnp.int32, (32, 128), 1)
    rim = (spot < 32) | (spot >= 96)
    for pair in range(2):
        span = slice(pair * 128, pair * 128 + 128)
        count = acc[512:544, span]
        for b in range(2):
            seen = pltpu.roll(count, 64, 1) if b else count
            hit = rim & (seen > 0.5)
            x = 4 * pair + 2 * b
            for v in range(8):
                new = acc[v * 32 : v * 32 + 32, span] + acc[256 + v * 32 : 288 + v * 32, span]
                if b:
                    new = pltpu.roll(new, 64, 1)
                old = state_ref[v, x : x + 2].reshape(32, 128)
                filled[v, x : x + 2] = jnp.where(hit, new, old).reshape(2, 16, 128)
    face_u[0] = filled[:, :, 0, :]
    face_u[1] = filled[:, :, 15, :]
    u_sides = side_copies(filled, face_u, u_x, u_y, u_send, u_recv)
    start_sides(u_sides)
    wait_sides(v_sides)
    wait_sides(u_sides)

    @pl.loop(0, chunks)
    def _(n):
        remote(first.at[n, 0:3], second.at[n, 0:3], y_send, y_recv.at[n], {"gx": i}).wait_send()
        mine = pl.ds(pl.multiple_of(n * 64, 64), 64)
        remote(third.at[mine], fourth.at[mine], d_send, d_recv.at[0], {"gx": i}).wait_send()


UNROLL = 4
PARTS = 2


def section(state, velocity, corner, frac, target):
    dma = pltpu.SemaphoreType.DMA
    chunk = pltpu.VMEM((6, 4, 16, 128), f32)
    whole = pltpu.VMEM((384, 128), f32)
    return pl.pallas_call(
        section_kernel,
        out_shape=(
            jax.ShapeDtypeStruct((8, 8, 16, 128), f32),
            jax.ShapeDtypeStruct((2, 8, 16, 128), f32),
            jax.ShapeDtypeStruct((2, 8, 8, 128), f32),
            jax.ShapeDtypeStruct((2, 3, 16, 128), f32),
            jax.ShapeDtypeStruct((2, 3, 8, 128), f32),
        ),
        in_specs=[pl.BlockSpec(memory_space=pltpu.HBM)] * 5,
        out_specs=(VMEM,) * 5,
        scratch_shapes=[
            pltpu.VMEM((1024, 256), bf16),
            pltpu.VMEM((48, 128), jnp.int32),
            pltpu.VMEM((3, 48, 128), f32),
            [pltpu.VMEM((1024, 256), f32) for _ in range(UNROLL)],
            pltpu.VMEM((128, 128), f32),
            chunk,
            chunk,
            whole,
            whole,
            [pltpu.VMEM((544, 2048 // PARTS), bf16) for _ in range(PARTS)],
            pltpu.VMEM((256, 6144), bf16),
            pltpu.VMEM((544, 256), f32),
            pltpu.VMEM((3, 8, 256), jnp.int32),
            pltpu.VMEM((2, 8, 8, 128), f32),
            pltpu.VMEM((2, 3, 8, 128), f32),
            pltpu.VMEM((8, 8, 16, 128), f32),
            pltpu.VMEM((3, 8, 16, 128), f32),
            pltpu.VMEM((4, 32, 64), jnp.int32),
            pltpu.VMEM((3, 4, 32, 64), f32),
            pltpu.VMEM((4, 32, 64), jnp.int32),
            dma((5,)),
            pltpu.SemaphoreType.REGULAR,
            dma,
            dma((6,)),
            dma,
            dma((3,)),
            dma((4,)),
            dma((4,)),
            dma((4,)),
            dma((4,)),
        ],
        compiler_params=pltpu.CompilerParams(
            collective_id=0, has_side_effects=True, vmem_limit_bytes=24 << 20
        ),
        name="section",
    )(state, velocity, corner, frac, target)


def face_weights(low, high):
    wave_low = jnp.minimum(jnp.minimum(low, high) - signal_speed, 0.0)
    wave_high = jnp.maximum(jnp.maximum(low, high) + signal_speed, 0.0)
    scale = courant_number / (wave_high - wave_low)
    return (
        wave_high * (low - wave_low) * scale,
        wave_low * (wave_high - high) * scale,
    )


def step_kernel(u_ref, vel_ref, ux_ref, uy_ref, vx_ref, vy_ref, out_hbm, out_ref, sems):
    puts = [pltpu.make_async_copy(out_ref.at[:, x], out_hbm.at[:, x], sems.at[x]) for x in range(8)]
    i, j = lax.axis_index("gx"), lax.axis_index("gy")
    lane = lax.broadcasted_iota(jnp.int32, (16, 128), 1)
    line = lax.broadcasted_iota(jnp.int32, (16, 128), 0)
    keep_low_x, keep_high_x = i > 0, i < 15
    keep_low_y, keep_high_y = j > 0, j < 3

    def plane(ref, side, v, x):
        if x < 0:
            return jnp.where(keep_low_x, side[0, v], 0.0)
        if x > 7:
            return jnp.where(keep_high_x, side[1, v], 0.0)
        return ref[v, x]

    def row(side, which, v, x):
        keep = keep_high_y if which else keep_low_y
        return jnp.where(keep, side[which, v, x : x + 1, :], 0.0)

    def prev_z(a):
        return jnp.where(lane == 0, 0.0, pltpu.roll(a, 1, 1))

    def next_z(a):
        return jnp.where(lane == 127, 0.0, pltpu.roll(a, 127, 1))

    def prev_y(a, low):
        return jnp.where(line == 0, low, pltpu.roll(a, 1, 0))

    def next_y(a, high):
        return jnp.where(line == 15, high, pltpu.roll(a, 15, 0))

    def elec(b, v):
        return (v[2] * b[1] - v[1] * b[2], v[0] * b[2] - v[2] * b[0], v[1] * b[0] - v[0] * b[1])

    speed = [[plane(vel_ref, vx_ref, d, x) for d in range(3)] for x in range(-1, 9)]
    weights_x = [face_weights(speed[x][0], speed[x + 1][0]) for x in range(9)]
    fields = [
        elec([plane(u_ref, ux_ref, 5 + d, x) for d in range(3)], speed[x + 1]) for x in range(-1, 9)
    ]
    flux_low = [
        weights_x[0][0] * plane(u_ref, ux_ref, v, -1) + weights_x[0][1] * u_ref[v, 0]
        for v in range(5)
    ]
    for x in range(8):
        here = speed[x + 1]
        low_v = [row(vy_ref, 0, d, x) for d in range(3)]
        high_v = [row(vy_ref, 1, d, x) for d in range(3)]
        y_low = face_weights(prev_y(here[1], low_v[1]), here[1])
        y_high = face_weights(here[1], next_y(here[1], high_v[1]))
        z_low = face_weights(prev_z(here[2]), here[2])
        z_high = face_weights(here[2], next_z(here[2]))
        centre = (
            1.0
            + y_low[1] - y_high[0]
            + z_low[1] - z_high[0]
        )
        for v in range(5):
            u = u_ref[v, x]
            flux_high = weights_x[x + 1][0] * u + weights_x[x + 1][1] * plane(
                u_ref, ux_ref, v, x + 1
            )
            new = centre * u - (flux_high - flux_low[v])
            flux_low[v] = flux_high
            new = new + y_low[0] * prev_y(u, row(uy_ref, 0, v, x))
            new = new - y_high[1] * next_y(u, row(uy_ref, 1, v, x))
            new = new + z_low[0] * prev_z(u)
            new = new - z_high[1] * next_z(u)
            out_ref[v, x] = new
        below, e, above = fields[x], fields[x + 1], fields[x + 2]
        e_low = elec([row(uy_ref, 0, 5 + d, x) for d in range(3)], low_v)
        e_high = elec([row(uy_ref, 1, 5 + d, x) for d in range(3)], high_v)

        def along_y(d):
            return next_y(e[d], e_high[d]) - prev_y(e[d], e_low[d])

        def along_z(d):
            return next_z(e[d]) - prev_z(e[d])

        def along_x(d):
            return above[d] - below[d]

        half = 0.5 * courant_number
        out_ref[5, x] = u_ref[5, x] - half * (along_y(2) - along_z(1))
        out_ref[6, x] = u_ref[6, x] - half * (along_z(0) - along_x(2))
        out_ref[7, x] = u_ref[7, x] - half * (along_x(1) - along_y(0))
        puts[x].start()
    for put in puts:
        put.wait()


def step(u, vel, ux, uy, vx, vy):
    return pl.pallas_call(
        step_kernel,
        out_shape=jax.ShapeDtypeStruct((8, 8, 16, 128), f32),
        in_specs=[VMEM] * 6,
        out_specs=pl.BlockSpec(memory_space=pl.ANY),
        scratch_shapes=[pltpu.VMEM((8, 8, 16, 128), f32), pltpu.SemaphoreType.DMA((8,))],
        compiler_params=pltpu.CompilerParams(vmem_limit_bytes=8 << 20),
        name="step",
    )(u, vel, ux, uy, vx, vy)


def per_device(conserved, velocity, donor_corner, donor_fraction, target_cell):
    state = conserved[:, 0]
    speeds = velocity[:, 0]
    corner = donor_corner[0, 0, 0].transpose(0, 2, 1)
    frac = donor_fraction[:, 0, 0, 0].transpose(0, 1, 3, 2)
    target = target_cell[0, 0, 0].transpose(0, 2, 1)
    state, far_speeds, corner, frac, target = (
        pltpu.with_memory_space_constraint(x, pltpu.HBM) for x in (state, speeds, corner, frac, target)
    )
    filled, u_x, u_y, v_x, v_y = section(state, far_speeds, corner, frac, target)
    return step(filled, speeds, u_x, u_y, v_x, v_y)[:, None]


def solution(mesh):
    return jax.shard_map(
        per_device,
        mesh=mesh,
        in_specs=(
            P(None, "grp", "gx", "gy", None),
            P(None, "grp", "gx", "gy", None),
            P("grp", "gx", "gy", None, None, None),
            P(None, "grp", "gx", "gy", None, None, None),
            P("grp", "gx", "gy", None, None, None),
        ),
        out_specs=P(None, "grp", "gx", "gy", None),
        check_vma=False,
    )
```

```python
import jax
import jax.numpy as jnp
from jax import lax
from jax.experimental import pallas as pl
from jax.experimental.pallas import tpu as pltpu
from jax.sharding import PartitionSpec as P

signal_speed = 0.5
courant_number = 0.3
f32 = jnp.float32
bf16 = jnp.bfloat16
MESH = pl.DeviceIdType.MESH
VMEM = pl.BlockSpec(memory_space=pltpu.VMEM)


def halves(x):
    head = x.astype(bf16)
    return head, (x - head.astype(f32)).astype(bf16)


def grid_step(k):
    return 1 + lax.rem(k + 1, 3)


def meetings(g):
    return 3 - g // 2


def send_slot(g, m):
    return m * (1 + g // 3)


def take_slot(g, m):
    return m * (1 + (g // 2) * (3 - g))


def packed_rows(block):
    return jnp.concatenate([block[8 * u : 8 * u + 8] for u in range(4)], axis=1)


def neighbours():
    i, j = lax.axis_index("gx"), lax.axis_index("gy")
    return (
        {"gx": lax.rem(i + 1, 16)},
        {"gx": lax.rem(i + 15, 16)},
        {"gy": lax.rem(j + 1, 4)},
        {"gy": lax.rem(j + 3, 4)},
    )


def side_copies(face_x, face_y, land_x, land_y, send, recv):
    pairs = (
        (face_x.at[:, 7], land_x.at[0]),
        (face_x.at[:, 0], land_x.at[1]),
        (face_y.at[1], land_y.at[0]),
        (face_y.at[0], land_y.at[1]),
    )
    return [
        remote(src, dst, send.at[n], recv.at[n], where)
        for n, ((src, dst), where) in enumerate(zip(pairs, neighbours()))
    ]


def edges():
    i, j = lax.axis_index("gx"), lax.axis_index("gy")
    return i < 15, i > 0, j < 3, j > 0


def start_sides(copies):
    for copy, there in zip(copies, edges()):
        pl.when(there)(copy.start)


def wait_sides(copies):
    up_x, down_x, up_y, down_y = edges()
    for copy, sends, comes in zip(
        copies, (up_x, down_x, up_y, down_y), (down_x, up_x, down_y, up_y)
    ):
        pl.when(sends)(copy.wait_send)
        pl.when(comes)(copy.wait_recv)


def remote(src, dst, send, recv, where):
    return pltpu.make_async_remote_copy(
        src_ref=src,
        dst_ref=dst,
        send_sem=send,
        recv_sem=recv,
        device_id=where,
        device_id_type=MESH,
    )


def interpolate(n, t, lhs, ints, floats, prod, turned):
    def two(ref):
        return jnp.concatenate(
            [ref[pl.ds(n * 8 + 2 * t, 1), :], ref[pl.ds(n * 8 + 2 * t + 1, 1), :]], axis=1
        )

    base = two(ints)
    fx, fy, fz = (two(floats.at[d]) for d in range(3))
    cz = base & 127
    cy = (base >> 7) & 15
    cx = base >> 11
    iz = lax.broadcasted_iota(jnp.int32, (128, 256), 0)
    wz = jnp.where(iz == cz, 1.0 - fz, jnp.where(iz == cz + 1, fz, 0.0))
    z_head, z_rest = halves(wz)
    both = lhs[...]
    prod[...] = jnp.dot(
        both, jnp.concatenate([z_head, z_head], axis=0), preferred_element_type=f32
    ) + jnp.dot(both, jnp.concatenate([z_rest, z_rest], axis=0), preferred_element_type=f32)
    iy = lax.broadcasted_iota(jnp.int32, (16, 256), 0)
    wy = jnp.where(iy == cy, 1.0 - fy, jnp.where(iy == cy + 1, fy, 0.0))
    wx = [jnp.where(cx == x, 1.0 - fx, jnp.where(cx + 1 == x, fx, 0.0)) for x in range(8)]
    rows = []
    for v in range(8):
        total = prod[v * 128 : v * 128 + 16, :] * wx[0]
        for x in range(1, 8):
            start = v * 128 + x * 16
            total = total + prod[start : start + 16, :] * wx[x]
        rows.append(jnp.sum(total * wy, axis=0, keepdims=True))
    values = jnp.concatenate(rows, axis=0)
    turned[pl.ds(pl.multiple_of(t * 16, 16), 16), :] = jnp.concatenate(
        [values[:, 0:128], values[:, 128:256]], axis=0
    )


def spots(ints, rr):
    cell = ints[pl.ds(rr, 1), :]
    column = cell >> 7
    lane = ((column >> 6) << 7) + (((cell & 127) + ((column & 32) << 1)) & 127)
    return column & 31, lane


def section_kernel(
    state_in, vel_in, corner_in, frac_in, target_in,
    filled, u_x, u_y, v_x, v_y,
    lhs, ints, floats, prods, turned, first, second, third, fourth, put_rows, put_lanes, acc, cells,
    face_u, face_v, state_ref, vel_ref, corner_ref, frac_ref, target_ref, loads,
    ready, y_send, y_recv, d_send, d_recv, v_send, v_recv, u_send, u_recv,
):
    g, i, j = lax.axis_index("grp"), lax.axis_index("gx"), lax.axis_index("gy")
    state_load, corner_load, frac_load, vel_load, target_load = (
        pltpu.make_async_copy(src, dst, loads.at[n])
        for n, (src, dst) in enumerate(
            (
                (state_in, state_ref),
                (corner_in, corner_ref),
                (frac_in, frac_ref),
                (vel_in, vel_ref),
                (target_in, target_ref),
            )
        )
    )
    for load in (corner_load, frac_load, state_load, vel_load, target_load):
        load.start()
    barrier = pltpu.get_barrier_semaphore()

    met = meetings(g)

    early = (15 - i) // 8
    grids = [lax.rem(g + grid_step(send_slot(g, m)), 4) for m in range(3)]

    def greet(m, semaphore, first_to):
        @pl.loop(0, 8, unroll=8)
        def _(to):
            where = {"grp": grids[m], "gx": first_to + to}
            pl.semaphore_signal(semaphore, inc=1, device_id=where, device_id_type=MESH)

    def greet_half(semaphore, first_to):
        greet(0, semaphore, first_to)
        greet(1, semaphore, first_to)

        @pl.when(met == 3)
        def _():
            greet(2, semaphore, first_to)

    @pl.when(early == 1)
    def _():
        greet_half(barrier, 0)

    greet_half(barrier, 8)
    for d in range(1, 4):
        where = {"gy": lax.rem(j + d, 4)}
        pl.semaphore_signal(barrier, inc=1, device_id=where, device_id_type=MESH)

    @pl.when(i < 15)
    def _():
        pl.semaphore_signal(barrier, inc=1, device_id={"gx": i + 1}, device_id_type=MESH)

    @pl.when(i > 0)
    def _():
        pl.semaphore_signal(barrier, inc=1, device_id={"gx": i - 1}, device_id_type=MESH)

    greeted = 8 * met * (2 - early) + 5 - (15 - i) // 15 - i // 15

    corner_load.wait()
    frac_load.wait()
    @pl.loop(0, met)
    def _(m):
        h = lax.rem(g + grid_step(send_slot(g, m)), 4)
        for c in range(2):
            at = pl.ds(pl.multiple_of((c * met + m) * 8, 8), 8)
            here = slice(32 * c, 32 * c + 32)
            ints[at, :] = packed_rows(corner_ref[h, :, here])
            for d in range(3):
                floats[d, at, :] = packed_rows(frac_ref[d, h, :, here])

    state_load.wait()
    head, rest = halves(state_ref[...].reshape(1024, 128))
    lhs[:, 0:128] = head
    lhs[:, 128:256] = rest
    v_sides = side_copies(vel_ref, face_v, v_x, v_y, v_send, v_recv)

    def onward(n):
        remote(first.at[n, 0:3], second.at[n, 0:3], y_send, y_recv.at[n], {"gx": i}).wait_recv()
        for came in range(4):
            for u in range(2):
                third[pl.ds(n * 64 + u * 4 + came, 8, stride=8), :] = second[
                    n, came, u * 8 : u * 8 + 8
                ]
        c = n // met
        k = send_slot(g, n - c * met)

        grid = lax.rem(g + grid_step(k), 4)

        @pl.loop(0, 8, unroll=8)
        def _(to):
            where = {"grp": grid, "gx": c * 8 + to}
            remote(
                third.at[pl.ds(pl.multiple_of(n * 64 + to * 8, 8), 8)],
                fourth.at[pl.ds(pl.multiple_of(k * 128 + i * 8, 8), 8)],
                d_send,
                d_recv.at[k],
                where,
            ).start()

    chunks = 2 * met
    wait_at = (met - 1) * early

    @pl.loop(0, chunks)
    def _(n):
        @pl.loop(0, 4 // len(prods))
        def _(step):
            for m, prod in enumerate(prods):
                interpolate(n, step * len(prods) + m, lhs, ints, floats, prod, turned)

        both = jnp.concatenate([turned[0:64, 0:64], turned[0:64, 64:128]], axis=0)
        turned[0:64, :] = both.T
        for to in range(4):
            first[n, to] = turned[pl.ds(to, 16, stride=4), :]
        second[n, j] = first[n, j]

        @pl.when(n == wait_at)
        def _():
            pl.semaphore_wait(barrier, greeted)

            @pl.when(early == 0)
            def _():
                greet_half(ready, 0)

        def along(m):
            for d in range(1, 4):
                to = lax.rem(j + d, 4)
                remote(
                    first.at[m, to], second.at[m, j], y_send, y_recv.at[m], {"gy": to}
                ).start()

        @pl.when(n == wait_at)
        def _():
            pl.loop(0, n + 1)(along)

        @pl.when(n > wait_at)
        def _():
            along(n)

        @pl.when(n * early == met + 1)
        def _():
            pl.loop(0, met)(onward)

        @pl.when(n * (1 - early) == 3)
        def _():
            onward(0)

        @pl.when(n * (1 - early) >= 3)
        def _():
            onward(n - 2)

    target_load.wait()

    @pl.loop(0, met)
    def _(m):
        cells[m] = packed_rows(target_ref[lax.rem(g + 4 - grid_step(take_slot(g, m)), 4)])

    @pl.loop((chunks - 2) * (1 - early) + met * early, chunks)
    def _(n):
        @pl.when(n == met + chunks * (1 - early))
        def _():
            pl.semaphore_wait(ready, 8 * met)

        onward(n)

    vel_load.wait()
    face_v[0] = vel_ref[:, :, 0, :]
    face_v[1] = vel_ref[:, :, 15, :]
    start_sides(v_sides)

    @pl.loop(0, 8 * met)
    def _(n):
        k, rr = n // 8, lax.rem(n, 8)
        _, lane = spots(cells.at[k], rr)
        il = lax.broadcasted_iota(jnp.int32, (256, 256), 0)
        put_lanes[:, pl.ds(pl.multiple_of(n * 256, 256), 256)] = jnp.where(
            il == lane, 1.0, 0.0
        ).astype(bf16)

    acc[...] = jnp.zeros_like(acc)

    @pl.loop(0, met)
    def _(n):
        k = take_slot(g, n)
        mine = pl.ds(pl.multiple_of(k * 128, 128), 128)
        remote(third.at[mine], fourth.at[mine], d_send, d_recv.at[k], {"gx": i}).wait_recv()
        for u in range(2):
            for came in range(4):
                turned[pl.ds(u * 64 + came, 16, stride=4), :] = fourth[
                    pl.ds(k * 128 + u * 4 + came, 16, stride=8), :
                ]
        turned[...] = turned[...].T
        for part, put in enumerate(put_rows):
            for m in range(8 // len(put_rows)):
                r = part * (8 // len(put_rows)) + m
                row, _ = spots(cells.at[n], r)
                values = jnp.concatenate(
                    [turned[r * 8 : r * 8 + 8, :], turned[64 + r * 8 : 72 + r * 8, :]], axis=1
                )
                head = values.astype(bf16).astype(f32)
                rest = values - head
                hit = lax.broadcasted_iota(jnp.int32, (32, 256), 0) == row
                at = slice(m * 256, m * 256 + 256)
                for v in range(8):
                    put[v * 32 : v * 32 + 32, at] = jnp.where(hit, head[v : v + 1, :], 0.0).astype(
                        bf16
                    )
                    put[256 + v * 32 : 288 + v * 32, at] = jnp.where(
                        hit, rest[v : v + 1, :], 0.0
                    ).astype(bf16)
                put[512:544, at] = jnp.where(hit, 1.0, 0.0).astype(bf16)
            span = 2048 // len(put_rows)
            acc[...] += lax.dot_general(
                put[...],
                put_lanes[:, pl.ds(pl.multiple_of(n * 2048 + part * span, span), span)],
                (((1,), (1,)), ((), ())),
                preferred_element_type=f32,
            )

    spot = lax.broadcasted_iota(jnp.int32, (32, 128), 1)
    rim = (spot < 32) | (spot >= 96)
    for pair in range(2):
        span = slice(pair * 128, pair * 128 + 128)
        count = acc[512:544, span]
        for b in range(2):
            seen = pltpu.roll(count, 64, 1) if b else count
            hit = rim & (seen > 0.5)
            x = 4 * pair + 2 * b
            for v in range(8):
                new = acc[v * 32 : v * 32 + 32, span] + acc[256 + v * 32 : 288 + v * 32, span]
                if b:
                    new = pltpu.roll(new, 64, 1)
                old = state_ref[v, x : x + 2].reshape(32, 128)
                filled[v, x : x + 2] = jnp.where(hit, new, old).reshape(2, 16, 128)
    face_u[0] = filled[:, :, 0, :]
    face_u[1] = filled[:, :, 15, :]
    u_sides = side_copies(filled, face_u, u_x, u_y, u_send, u_recv)
    start_sides(u_sides)
    wait_sides(v_sides)
    wait_sides(u_sides)

    @pl.loop(0, chunks)
    def _(n):
        remote(first.at[n, 0:3], second.at[n, 0:3], y_send, y_recv.at[n], {"gx": i}).wait_send()
        mine = pl.ds(pl.multiple_of(n * 64, 64), 64)
        remote(third.at[mine], fourth.at[mine], d_send, d_recv.at[0], {"gx": i}).wait_send()


UNROLL = 4
PARTS = 2


def section(state, velocity, corner, frac, target):
    dma = pltpu.SemaphoreType.DMA
    chunk = pltpu.VMEM((6, 4, 16, 128), f32)
    whole = pltpu.VMEM((384, 128), f32)
    return pl.pallas_call(
        section_kernel,
        out_shape=(
            jax.ShapeDtypeStruct((8, 8, 16, 128), f32),
            jax.ShapeDtypeStruct((2, 8, 16, 128), f32),
            jax.ShapeDtypeStruct((2, 8, 8, 128), f32),
            jax.ShapeDtypeStruct((2, 3, 16, 128), f32),
            jax.ShapeDtypeStruct((2, 3, 8, 128), f32),
        ),
        in_specs=[pl.BlockSpec(memory_space=pltpu.HBM)] * 5,
        out_specs=(VMEM,) * 5,
        scratch_shapes=[
            pltpu.VMEM((1024, 256), bf16),
            pltpu.VMEM((48, 128), jnp.int32),
            pltpu.VMEM((3, 48, 128), f32),
            [pltpu.VMEM((1024, 256), f32) for _ in range(UNROLL)],
            pltpu.VMEM((128, 128), f32),
            chunk,
            chunk,
            whole,
            whole,
            [pltpu.VMEM((544, 2048 // PARTS), bf16) for _ in range(PARTS)],
            pltpu.VMEM((256, 6144), bf16),
            pltpu.VMEM((544, 256), f32),
            pltpu.VMEM((3, 8, 256), jnp.int32),
            pltpu.VMEM((2, 8, 8, 128), f32),
            pltpu.VMEM((2, 3, 8, 128), f32),
            pltpu.VMEM((8, 8, 16, 128), f32),
            pltpu.VMEM((3, 8, 16, 128), f32),
            pltpu.VMEM((4, 32, 64), jnp.int32),
            pltpu.VMEM((3, 4, 32, 64), f32),
            pltpu.VMEM((4, 32, 64), jnp.int32),
            dma((5,)),
            pltpu.SemaphoreType.REGULAR,
            dma,
            dma((6,)),
            dma,
            dma((3,)),
            dma((4,)),
            dma((4,)),
            dma((4,)),
            dma((4,)),
        ],
        compiler_params=pltpu.CompilerParams(
            collective_id=0, has_side_effects=True, vmem_limit_bytes=24 << 20
        ),
        name="section",
    )(state, velocity, corner, frac, target)


def face_weights(low, high):
    wave_low = jnp.minimum(jnp.minimum(low, high) - signal_speed, 0.0)
    wave_high = jnp.maximum(jnp.maximum(low, high) + signal_speed, 0.0)
    scale = courant_number / (wave_high - wave_low)
    return (
        wave_high * (low - wave_low) * scale,
        wave_low * (wave_high - high) * scale,
    )


def step_kernel(u_ref, vel_ref, ux_ref, uy_ref, vx_ref, vy_ref, out_hbm, out_ref, sems):
    puts = [pltpu.make_async_copy(out_ref.at[:, x], out_hbm.at[:, x], sems.at[x]) for x in range(8)]
    i, j = lax.axis_index("gx"), lax.axis_index("gy")
    lane = lax.broadcasted_iota(jnp.int32, (16, 128), 1)
    line = lax.broadcasted_iota(jnp.int32, (16, 128), 0)
    keep_low_x, keep_high_x = i > 0, i < 15
    keep_low_y, keep_high_y = j > 0, j < 3

    def plane(ref, side, v, x):
        if x < 0:
            return jnp.where(keep_low_x, side[0, v], 0.0)
        if x > 7:
            return jnp.where(keep_high_x, side[1, v], 0.0)
        return ref[v, x]

    def row(side, which, v, x):
        keep = keep_high_y if which else keep_low_y
        return jnp.where(keep, side[which, v, x : x + 1, :], 0.0)

    def prev_z(a):
        return jnp.where(lane == 0, 0.0, pltpu.roll(a, 1, 1))

    def next_z(a):
        return jnp.where(lane == 127, 0.0, pltpu.roll(a, 127, 1))

    def prev_y(a, low):
        return jnp.where(line == 0, low, pltpu.roll(a, 1, 0))

    def next_y(a, high):
        return jnp.where(line == 15, high, pltpu.roll(a, 15, 0))

    def elec(b, v):
        return (v[2] * b[1] - v[1] * b[2], v[0] * b[2] - v[2] * b[0], v[1] * b[0] - v[0] * b[1])

    speed = [[plane(vel_ref, vx_ref, d, x) for d in range(3)] for x in range(-1, 9)]
    weights_x = [face_weights(speed[x][0], speed[x + 1][0]) for x in range(9)]
    fields = [
        elec([plane(u_ref, ux_ref, 5 + d, x) for d in range(3)], speed[x + 1]) for x in range(-1, 9)
    ]
    flux_low = [
        weights_x[0][0] * plane(u_ref, ux_ref, v, -1) + weights_x[0][1] * u_ref[v, 0]
        for v in range(5)
    ]
    for x in range(8):
        here = speed[x + 1]
        low_v = [row(vy_ref, 0, d, x) for d in range(3)]
        high_v = [row(vy_ref, 1, d, x) for d in range(3)]
        y_low = face_weights(prev_y(here[1], low_v[1]), here[1])
        y_high = face_weights(here[1], next_y(here[1], high_v[1]))
        z_low = face_weights(prev_z(here[2]), here[2])
        z_high = face_weights(here[2], next_z(here[2]))
        centre = (
            1.0
            + y_low[1] - y_high[0]
            + z_low[1] - z_high[0]
        )
        for v in range(5):
            u = u_ref[v, x]
            flux_high = weights_x[x + 1][0] * u + weights_x[x + 1][1] * plane(
                u_ref, ux_ref, v, x + 1
            )
            new = centre * u - (flux_high - flux_low[v])
            flux_low[v] = flux_high
            new = new + y_low[0] * prev_y(u, row(uy_ref, 0, v, x))
            new = new - y_high[1] * next_y(u, row(uy_ref, 1, v, x))
            new = new + z_low[0] * prev_z(u)
            new = new - z_high[1] * next_z(u)
            out_ref[v, x] = new
        below, e, above = fields[x], fields[x + 1], fields[x + 2]
        e_low = elec([row(uy_ref, 0, 5 + d, x) for d in range(3)], low_v)
        e_high = elec([row(uy_ref, 1, 5 + d, x) for d in range(3)], high_v)

        def along_y(d):
            return next_y(e[d], e_high[d]) - prev_y(e[d], e_low[d])

        def along_z(d):
            return next_z(e[d]) - prev_z(e[d])

        def along_x(d):
            return above[d] - below[d]

        half = 0.5 * courant_number
        out_ref[5, x] = u_ref[5, x] - half * (along_y(2) - along_z(1))
        out_ref[6, x] = u_ref[6, x] - half * (along_z(0) - along_x(2))
        out_ref[7, x] = u_ref[7, x] - half * (along_x(1) - along_y(0))
        puts[x].start()
    for put in puts:
        put.wait()


def step(u, vel, ux, uy, vx, vy):
    return pl.pallas_call(
        step_kernel,
        out_shape=jax.ShapeDtypeStruct((8, 8, 16, 128), f32),
        in_specs=[VMEM] * 6,
        out_specs=pl.BlockSpec(memory_space=pl.ANY),
        scratch_shapes=[pltpu.VMEM((8, 8, 16, 128), f32), pltpu.SemaphoreType.DMA((8,))],
        compiler_params=pltpu.CompilerParams(vmem_limit_bytes=8 << 20),
        name="step",
    )(u, vel, ux, uy, vx, vy)


def per_device(conserved, velocity, donor_corner, donor_fraction, target_cell):
    state = conserved[:, 0]
    speeds = velocity[:, 0]
    corner = donor_corner[0, 0, 0].transpose(0, 2, 1)
    frac = donor_fraction[:, 0, 0, 0].transpose(0, 1, 3, 2)
    target = target_cell[0, 0, 0].transpose(0, 2, 1)
    state, far_speeds, corner, frac, target = (
        pltpu.with_memory_space_constraint(x, pltpu.HBM) for x in (state, speeds, corner, frac, target)
    )
    filled, u_x, u_y, v_x, v_y = section(state, far_speeds, corner, frac, target)
    return step(filled, speeds, u_x, u_y, v_x, v_y)[:, None]


def solution(mesh):
    return jax.shard_map(
        per_device,
        mesh=mesh,
        in_specs=(
            P(None, "grp", "gx", "gy", None),
            P(None, "grp", "gx", "gy", None),
            P("grp", "gx", "gy", None, None, None),
            P(None, "grp", "gx", "gy", None, None, None),
            P("grp", "gx", "gy", None, None, None),
        ),
        out_specs=P(None, "grp", "gx", "gy", None),
        check_vma=False,
    )
```

```python
import jax
import jax.numpy as jnp
from jax import lax
from jax.experimental import pallas as pl
from jax.experimental.pallas import tpu as pltpu
from jax.sharding import PartitionSpec as P

signal_speed = 0.5
courant_number = 0.3
f32 = jnp.float32
bf16 = jnp.bfloat16
MESH = pl.DeviceIdType.MESH
VMEM = pl.BlockSpec(memory_space=pltpu.VMEM)


def halves(x):
    head = x.astype(bf16)
    return head, (x - head.astype(f32)).astype(bf16)


def grid_step(k):
    return 1 + lax.rem(k + 1, 3)


def meetings(g):
    return 3 - g // 2


def send_slot(g, m):
    return m * (1 + g // 3)


def take_slot(g, m):
    return m * (1 + (g // 2) * (3 - g))


def packed_rows(block):
    return jnp.concatenate([block[8 * u : 8 * u + 8] for u in range(4)], axis=1)


def neighbours():
    i, j = lax.axis_index("gx"), lax.axis_index("gy")
    return (
        {"gx": lax.rem(i + 1, 16)},
        {"gx": lax.rem(i + 15, 16)},
        {"gy": lax.rem(j + 1, 4)},
        {"gy": lax.rem(j + 3, 4)},
    )


def side_copies(face_x, face_y, land_x, land_y, send, recv):
    pairs = (
        (face_x.at[:, 7], land_x.at[0]),
        (face_x.at[:, 0], land_x.at[1]),
        (face_y.at[1], land_y.at[0]),
        (face_y.at[0], land_y.at[1]),
    )
    return [
        remote(src, dst, send.at[n], recv.at[n], where)
        for n, ((src, dst), where) in enumerate(zip(pairs, neighbours()))
    ]


def edges():
    i, j = lax.axis_index("gx"), lax.axis_index("gy")
    return i < 15, i > 0, j < 3, j > 0


def start_sides(copies):
    for copy, there in zip(copies, edges()):
        pl.when(there)(copy.start)


def wait_sides(copies):
    up_x, down_x, up_y, down_y = edges()
    for copy, sends, comes in zip(
        copies, (up_x, down_x, up_y, down_y), (down_x, up_x, down_y, up_y)
    ):
        pl.when(sends)(copy.wait_send)
        pl.when(comes)(copy.wait_recv)


def remote(src, dst, send, recv, where):
    return pltpu.make_async_remote_copy(
        src_ref=src,
        dst_ref=dst,
        send_sem=send,
        recv_sem=recv,
        device_id=where,
        device_id_type=MESH,
    )


def interpolate(n, t, lhs, ints, floats, prod, turned):
    def two(ref):
        return jnp.concatenate(
            [ref[pl.ds(n * 8 + 2 * t, 1), :], ref[pl.ds(n * 8 + 2 * t + 1, 1), :]], axis=1
        )

    base = two(ints)
    fx, fy, fz = (two(floats.at[d]) for d in range(3))
    cz = base & 127
    cy = (base >> 7) & 15
    cx = base >> 11
    iz = lax.broadcasted_iota(jnp.int32, (128, 256), 0)
    wz = jnp.where(iz == cz, 1.0 - fz, jnp.where(iz == cz + 1, fz, 0.0))
    z_head, z_rest = halves(wz)
    both = lhs[...]
    prod[...] = jnp.dot(
        both, jnp.concatenate([z_head, z_head], axis=0), preferred_element_type=f32
    ) + jnp.dot(both, jnp.concatenate([z_rest, z_rest], axis=0), preferred_element_type=f32)
    iy = lax.broadcasted_iota(jnp.int32, (16, 256), 0)
    wy = jnp.where(iy == cy, 1.0 - fy, jnp.where(iy == cy + 1, fy, 0.0))
    wx = [jnp.where(cx == x, 1.0 - fx, jnp.where(cx + 1 == x, fx, 0.0)) for x in range(8)]
    rows = []
    for v in range(8):
        total = prod[v * 128 : v * 128 + 16, :] * wx[0]
        for x in range(1, 8):
            start = v * 128 + x * 16
            total = total + prod[start : start + 16, :] * wx[x]
        rows.append(jnp.sum(total * wy, axis=0, keepdims=True))
    values = jnp.concatenate(rows, axis=0)
    turned[pl.ds(pl.multiple_of(t * 16, 16), 16), :] = jnp.concatenate(
        [values[:, 0:128], values[:, 128:256]], axis=0
    )


def spots(ints, rr):
    cell = ints[pl.ds(rr, 1), :]
    column = cell >> 7
    lane = ((column >> 6) << 7) + (((cell & 127) + ((column & 32) << 1)) & 127)
    return column & 31, lane


def section_kernel(
    state_in, vel_in, corner_in, frac_in, target_in,
    filled, u_x, u_y, v_x, v_y,
    lhs, ints, floats, prods, turned, first, second, third, fourth, put_rows, put_lanes, acc, cells,
    face_u, face_v, state_ref, vel_ref, corner_ref, frac_ref, target_ref, loads,
    ready, y_send, y_recv, d_send, d_recv, v_send, v_recv, u_send, u_recv,
):
    g, i, j = lax.axis_index("grp"), lax.axis_index("gx"), lax.axis_index("gy")
    state_load, corner_load, frac_load, vel_load, target_load = (
        pltpu.make_async_copy(src, dst, loads.at[n])
        for n, (src, dst) in enumerate(
            (
                (state_in, state_ref),
                (corner_in, corner_ref),
                (frac_in, frac_ref),
                (vel_in, vel_ref),
                (target_in, target_ref),
            )
        )
    )
    for load in (corner_load, frac_load, state_load, vel_load, target_load):
        load.start()
    barrier = pltpu.get_barrier_semaphore()

    met = meetings(g)

    early = (15 - i) // 8
    grids = [lax.rem(g + grid_step(send_slot(g, m)), 4) for m in range(3)]

    def greet(m, semaphore, first_to):
        @pl.loop(0, 8, unroll=8)
        def _(to):
            where = {"grp": grids[m], "gx": first_to + to}
            pl.semaphore_signal(semaphore, inc=1, device_id=where, device_id_type=MESH)

    def greet_half(semaphore, first_to):
        greet(0, semaphore, first_to)
        greet(1, semaphore, first_to)

        @pl.when(met == 3)
        def _():
            greet(2, semaphore, first_to)

    @pl.when(early == 1)
    def _():
        greet_half(barrier, 0)

    greet_half(barrier, 8)
    for d in range(1, 4):
        where = {"gy": lax.rem(j + d, 4)}
        pl.semaphore_signal(barrier, inc=1, device_id=where, device_id_type=MESH)

    @pl.when(i < 15)
    def _():
        pl.semaphore_signal(barrier, inc=1, device_id={"gx": i + 1}, device_id_type=MESH)

    @pl.when(i > 0)
    def _():
        pl.semaphore_signal(barrier, inc=1, device_id={"gx": i - 1}, device_id_type=MESH)

    greeted = 8 * met * (2 - early) + 5 - (15 - i) // 15 - i // 15

    corner_load.wait()
    frac_load.wait()
    @pl.loop(0, met)
    def _(m):
        h = lax.rem(g + grid_step(send_slot(g, m)), 4)
        for c in range(2):
            at = pl.ds(pl.multiple_of((c * met + m) * 8, 8), 8)
            here = slice(32 * c, 32 * c + 32)
            ints[at, :] = packed_rows(corner_ref[h, :, here])
            for d in range(3):
                floats[d, at, :] = packed_rows(frac_ref[d, h, :, here])

    state_load.wait()
    head, rest = halves(state_ref[...].reshape(1024, 128))
    lhs[:, 0:128] = head
    lhs[:, 128:256] = rest
    v_sides = side_copies(vel_ref, face_v, v_x, v_y, v_send, v_recv)

    def onward(n):
        remote(first.at[n, 0:3], second.at[n, 0:3], y_send, y_recv.at[n], {"gx": i}).wait_recv()
        for came in range(4):
            for u in range(2):
                third[pl.ds(n * 64 + u * 4 + came, 8, stride=8), :] = second[
                    n, came, u * 8 : u * 8 + 8
                ]
        c = n // met
        k = send_slot(g, n - c * met)

        grid = lax.rem(g + grid_step(k), 4)

        @pl.loop(0, 8, unroll=8)
        def _(to):
            where = {"grp": grid, "gx": c * 8 + to}
            remote(
                third.at[pl.ds(pl.multiple_of(n * 64 + to * 8, 8), 8)],
                fourth.at[pl.ds(pl.multiple_of(k * 128 + i * 8, 8), 8)],
                d_send,
                d_recv.at[k],
                where,
            ).start()

    chunks = 2 * met
    wait_at = (met - 1) * early

    @pl.loop(0, chunks)
    def _(n):
        @pl.loop(0, 4 // len(prods))
        def _(step):
            for m, prod in enumerate(prods):
                interpolate(n, step * len(prods) + m, lhs, ints, floats, prod, turned)

        both = jnp.concatenate([turned[0:64, 0:64], turned[0:64, 64:128]], axis=0)
        turned[0:64, :] = both.T
        for to in range(4):
            first[n, to] = turned[pl.ds(to, 16, stride=4), :]
        second[n, j] = first[n, j]

        @pl.when(n == wait_at)
        def _():
            pl.semaphore_wait(barrier, greeted)

        def along(m):
            for d in range(1, 4):
                to = lax.rem(j + d, 4)
                remote(
                    first.at[m, to], second.at[m, j], y_send, y_recv.at[m], {"gy": to}
                ).start()

        @pl.when(n == wait_at)
        def _():
            pl.loop(0, n + 1)(along)

            @pl.when(early == 0)
            def _():
                greet_half(ready, 0)

        @pl.when(n > wait_at)
        def _():
            along(n)

        @pl.when(n * early == met + 1)
        def _():
            pl.loop(0, met)(onward)

        @pl.when(n * (1 - early) >= 2)
        def _():
            onward(n - 2)

    target_load.wait()

    @pl.loop(0, met)
    def _(m):
        cells[m] = packed_rows(target_ref[lax.rem(g + 4 - grid_step(take_slot(g, m)), 4)])

    @pl.loop((chunks - 2) * (1 - early) + met * early, chunks)
    def _(n):
        @pl.when(n == met + chunks * (1 - early))
        def _():
            pl.semaphore_wait(ready, 8 * met)

        onward(n)

    vel_load.wait()
    face_v[0] = vel_ref[:, :, 0, :]
    face_v[1] = vel_ref[:, :, 15, :]
    start_sides(v_sides)

    @pl.loop(0, 8 * met)
    def _(n):
        k, rr = n // 8, lax.rem(n, 8)
        _, lane = spots(cells.at[k], rr)
        il = lax.broadcasted_iota(jnp.int32, (256, 256), 0)
        put_lanes[:, pl.ds(pl.multiple_of(n * 256, 256), 256)] = jnp.where(
            il == lane, 1.0, 0.0
        ).astype(bf16)

    acc[...] = jnp.zeros_like(acc)

    @pl.loop(0, met)
    def _(n):
        k = take_slot(g, n)
        mine = pl.ds(pl.multiple_of(k * 128, 128), 128)
        remote(third.at[mine], fourth.at[mine], d_send, d_recv.at[k], {"gx": i}).wait_recv()
        for u in range(2):
            for came in range(4):
                turned[pl.ds(u * 64 + came, 16, stride=4), :] = fourth[
                    pl.ds(k * 128 + u * 4 + came, 16, stride=8), :
                ]
        turned[...] = turned[...].T
        for part, put in enumerate(put_rows):
            for m in range(8 // len(put_rows)):
                r = part * (8 // len(put_rows)) + m
                row, _ = spots(cells.at[n], r)
                values = jnp.concatenate(
                    [turned[r * 8 : r * 8 + 8, :], turned[64 + r * 8 : 72 + r * 8, :]], axis=1
                )
                head = values.astype(bf16).astype(f32)
                rest = values - head
                hit = lax.broadcasted_iota(jnp.int32, (32, 256), 0) == row
                at = slice(m * 256, m * 256 + 256)
                for v in range(8):
                    put[v * 32 : v * 32 + 32, at] = jnp.where(hit, head[v : v + 1, :], 0.0).astype(
                        bf16
                    )
                    put[256 + v * 32 : 288 + v * 32, at] = jnp.where(
                        hit, rest[v : v + 1, :], 0.0
                    ).astype(bf16)
                put[512:544, at] = jnp.where(hit, 1.0, 0.0).astype(bf16)
            span = 2048 // len(put_rows)
            acc[...] += lax.dot_general(
                put[...],
                put_lanes[:, pl.ds(pl.multiple_of(n * 2048 + part * span, span), span)],
                (((1,), (1,)), ((), ())),
                preferred_element_type=f32,
            )

    spot = lax.broadcasted_iota(jnp.int32, (32, 128), 1)
    rim = (spot < 32) | (spot >= 96)
    for pair in range(2):
        span = slice(pair * 128, pair * 128 + 128)
        count = acc[512:544, span]
        for b in range(2):
            seen = pltpu.roll(count, 64, 1) if b else count
            hit = rim & (seen > 0.5)
            x = 4 * pair + 2 * b
            for v in range(8):
                new = acc[v * 32 : v * 32 + 32, span] + acc[256 + v * 32 : 288 + v * 32, span]
                if b:
                    new = pltpu.roll(new, 64, 1)
                old = state_ref[v, x : x + 2].reshape(32, 128)
                filled[v, x : x + 2] = jnp.where(hit, new, old).reshape(2, 16, 128)
    face_u[0] = filled[:, :, 0, :]
    face_u[1] = filled[:, :, 15, :]
    u_sides = side_copies(filled, face_u, u_x, u_y, u_send, u_recv)
    start_sides(u_sides)
    wait_sides(v_sides)
    wait_sides(u_sides)

    @pl.loop(0, chunks)
    def _(n):
        remote(first.at[n, 0:3], second.at[n, 0:3], y_send, y_recv.at[n], {"gx": i}).wait_send()
        mine = pl.ds(pl.multiple_of(n * 64, 64), 64)
        remote(third.at[mine], fourth.at[mine], d_send, d_recv.at[0], {"gx": i}).wait_send()


UNROLL = 4
PARTS = 2


def section(state, velocity, corner, frac, target):
    dma = pltpu.SemaphoreType.DMA
    chunk = pltpu.VMEM((6, 4, 16, 128), f32)
    whole = pltpu.VMEM((384, 128), f32)
    return pl.pallas_call(
        section_kernel,
        out_shape=(
            jax.ShapeDtypeStruct((8, 8, 16, 128), f32),
            jax.ShapeDtypeStruct((2, 8, 16, 128), f32),
            jax.ShapeDtypeStruct((2, 8, 8, 128), f32),
            jax.ShapeDtypeStruct((2, 3, 16, 128), f32),
            jax.ShapeDtypeStruct((2, 3, 8, 128), f32),
        ),
        in_specs=[pl.BlockSpec(memory_space=pltpu.HBM)] * 5,
        out_specs=(VMEM,) * 5,
        scratch_shapes=[
            pltpu.VMEM((1024, 256), bf16),
            pltpu.VMEM((48, 128), jnp.int32),
            pltpu.VMEM((3, 48, 128), f32),
            [pltpu.VMEM((1024, 256), f32) for _ in range(UNROLL)],
            pltpu.VMEM((128, 128), f32),
            chunk,
            chunk,
            whole,
            whole,
            [pltpu.VMEM((544, 2048 // PARTS), bf16) for _ in range(PARTS)],
            pltpu.VMEM((256, 6144), bf16),
            pltpu.VMEM((544, 256), f32),
            pltpu.VMEM((3, 8, 256), jnp.int32),
            pltpu.VMEM((2, 8, 8, 128), f32),
            pltpu.VMEM((2, 3, 8, 128), f32),
            pltpu.VMEM((8, 8, 16, 128), f32),
            pltpu.VMEM((3, 8, 16, 128), f32),
            pltpu.VMEM((4, 32, 64), jnp.int32),
            pltpu.VMEM((3, 4, 32, 64), f32),
            pltpu.VMEM((4, 32, 64), jnp.int32),
            dma((5,)),
            pltpu.SemaphoreType.REGULAR,
            dma,
            dma((6,)),
            dma,
            dma((3,)),
            dma((4,)),
            dma((4,)),
            dma((4,)),
            dma((4,)),
        ],
        compiler_params=pltpu.CompilerParams(
            collective_id=0, has_side_effects=True, vmem_limit_bytes=24 << 20
        ),
        name="section",
    )(state, velocity, corner, frac, target)


def face_weights(low, high):
    wave_low = jnp.minimum(jnp.minimum(low, high) - signal_speed, 0.0)
    wave_high = jnp.maximum(jnp.maximum(low, high) + signal_speed, 0.0)
    scale = courant_number / (wave_high - wave_low)
    return (
        wave_high * (low - wave_low) * scale,
        wave_low * (wave_high - high) * scale,
    )


def step_kernel(u_ref, vel_ref, ux_ref, uy_ref, vx_ref, vy_ref, out_hbm, out_ref, sems):
    puts = [pltpu.make_async_copy(out_ref.at[:, x], out_hbm.at[:, x], sems.at[x]) for x in range(8)]
    i, j = lax.axis_index("gx"), lax.axis_index("gy")
    lane = lax.broadcasted_iota(jnp.int32, (16, 128), 1)
    line = lax.broadcasted_iota(jnp.int32, (16, 128), 0)
    keep_low_x, keep_high_x = i > 0, i < 15
    keep_low_y, keep_high_y = j > 0, j < 3

    def plane(ref, side, v, x):
        if x < 0:
            return jnp.where(keep_low_x, side[0, v], 0.0)
        if x > 7:
            return jnp.where(keep_high_x, side[1, v], 0.0)
        return ref[v, x]

    def row(side, which, v, x):
        keep = keep_high_y if which else keep_low_y
        return jnp.where(keep, side[which, v, x : x + 1, :], 0.0)

    def prev_z(a):
        return jnp.where(lane == 0, 0.0, pltpu.roll(a, 1, 1))

    def next_z(a):
        return jnp.where(lane == 127, 0.0, pltpu.roll(a, 127, 1))

    def prev_y(a, low):
        return jnp.where(line == 0, low, pltpu.roll(a, 1, 0))

    def next_y(a, high):
        return jnp.where(line == 15, high, pltpu.roll(a, 15, 0))

    def elec(b, v):
        return (v[2] * b[1] - v[1] * b[2], v[0] * b[2] - v[2] * b[0], v[1] * b[0] - v[0] * b[1])

    speed = [[plane(vel_ref, vx_ref, d, x) for d in range(3)] for x in range(-1, 9)]
    weights_x = [face_weights(speed[x][0], speed[x + 1][0]) for x in range(9)]
    fields = [
        elec([plane(u_ref, ux_ref, 5 + d, x) for d in range(3)], speed[x + 1]) for x in range(-1, 9)
    ]
    flux_low = [
        weights_x[0][0] * plane(u_ref, ux_ref, v, -1) + weights_x[0][1] * u_ref[v, 0]
        for v in range(5)
    ]
    for x in range(8):
        here = speed[x + 1]
        low_v = [row(vy_ref, 0, d, x) for d in range(3)]
        high_v = [row(vy_ref, 1, d, x) for d in range(3)]
        y_low = face_weights(prev_y(here[1], low_v[1]), here[1])
        y_high = face_weights(here[1], next_y(here[1], high_v[1]))
        z_low = face_weights(prev_z(here[2]), here[2])
        z_high = face_weights(here[2], next_z(here[2]))
        centre = (
            1.0
            + y_low[1] - y_high[0]
            + z_low[1] - z_high[0]
        )
        for v in range(5):
            u = u_ref[v, x]
            flux_high = weights_x[x + 1][0] * u + weights_x[x + 1][1] * plane(
                u_ref, ux_ref, v, x + 1
            )
            new = centre * u - (flux_high - flux_low[v])
            flux_low[v] = flux_high
            new = new + y_low[0] * prev_y(u, row(uy_ref, 0, v, x))
            new = new - y_high[1] * next_y(u, row(uy_ref, 1, v, x))
            new = new + z_low[0] * prev_z(u)
            new = new - z_high[1] * next_z(u)
            out_ref[v, x] = new
        below, e, above = fields[x], fields[x + 1], fields[x + 2]
        e_low = elec([row(uy_ref, 0, 5 + d, x) for d in range(3)], low_v)
        e_high = elec([row(uy_ref, 1, 5 + d, x) for d in range(3)], high_v)

        def along_y(d):
            return next_y(e[d], e_high[d]) - prev_y(e[d], e_low[d])

        def along_z(d):
            return next_z(e[d]) - prev_z(e[d])

        def along_x(d):
            return above[d] - below[d]

        half = 0.5 * courant_number
        out_ref[5, x] = u_ref[5, x] - half * (along_y(2) - along_z(1))
        out_ref[6, x] = u_ref[6, x] - half * (along_z(0) - along_x(2))
        out_ref[7, x] = u_ref[7, x] - half * (along_x(1) - along_y(0))
        puts[x].start()
    for put in puts:
        put.wait()


def step(u, vel, ux, uy, vx, vy):
    return pl.pallas_call(
        step_kernel,
        out_shape=jax.ShapeDtypeStruct((8, 8, 16, 128), f32),
        in_specs=[VMEM] * 6,
        out_specs=pl.BlockSpec(memory_space=pl.ANY),
        scratch_shapes=[pltpu.VMEM((8, 8, 16, 128), f32), pltpu.SemaphoreType.DMA((8,))],
        compiler_params=pltpu.CompilerParams(vmem_limit_bytes=8 << 20),
        name="step",
    )(u, vel, ux, uy, vx, vy)


def per_device(conserved, velocity, donor_corner, donor_fraction, target_cell):
    state = conserved[:, 0]
    speeds = velocity[:, 0]
    corner = donor_corner[0, 0, 0].transpose(0, 2, 1)
    frac = donor_fraction[:, 0, 0, 0].transpose(0, 1, 3, 2)
    target = target_cell[0, 0, 0].transpose(0, 2, 1)
    state, far_speeds, corner, frac, target = (
        pltpu.with_memory_space_constraint(x, pltpu.HBM) for x in (state, speeds, corner, frac, target)
    )
    filled, u_x, u_y, v_x, v_y = section(state, far_speeds, corner, frac, target)
    return step(filled, speeds, u_x, u_y, v_x, v_y)[:, None]


def solution(mesh):
    return jax.shard_map(
        per_device,
        mesh=mesh,
        in_specs=(
            P(None, "grp", "gx", "gy", None),
            P(None, "grp", "gx", "gy", None),
            P("grp", "gx", "gy", None, None, None),
            P(None, "grp", "gx", "gy", None, None, None),
            P("grp", "gx", "gy", None, None, None),
        ),
        out_specs=P(None, "grp", "gx", "gy", None),
        check_vma=False,
    )
```
